256 devices in a mesh: cp: 64 (over z, x, core), tp: 4 (over y).
Axes of the slice: x: 4, y: 4, z: 8, core: 2. Of those that a mesh axis runs over, the one named last changes fastest.
Arguments:
- queries: bfloat16 [8192, 8192], P('cp', 'tp'), may hold values from -6 to 6
- keys: bfloat16 [8192, 1024], P('cp', 'tp'), may hold values from -6 to 6
- values: bfloat16 [8192, 1024], P('cp', 'tp'), may hold values from -6 to 6
- doc_blocks: int32 [4], replicated, may hold values from 1 to 32, 64 in all
- block_order: int32 [64], replicated, may hold values from 0 to 63, each once
- out_weight: bfloat16 [8192, 4096], P('tp'), may hold values from -0.5 to 0.5
Outputs:
- layer_out: bfloat16 [8192, 4096], P(('cp', 'tp'))
The draws below stay inside these ranges and needn't reach their ends.
Inputs may be any that keep to these rules, and one draw needn't show every extreme that they name: Array block i (rows i * 128 to i * 128 + 127) holds sequence block block_order[i]; every block number appears once. `doc_blocks`: they sum to 64; the longest document has exactly 32 blocks.
All inputs are finite; a program needn't handle non-finite values.
Results may differ from the reference program's by a relative error of at most 0.013.
Values may be sent and summed in bfloat16 or wider, within the bound.
A program may use at most 128 MiB of HBM per device.

```python
import math
import jax
import jax.numpy as jnp
import numpy as np
from jax import lax

QUERY_HEADS = 64
KEY_VALUE_HEADS = 8
HEAD_SIZE = 128
WIN = 4096
BLOCK_TOKENS = 128
NDOC = 4
GROUP_HEADS = 8
PACK_TOKENS = 8192
NBLK = 64
MOSTB = 32


def draw_keys(key, part):
    picked_rows = jax.random.truncated_normal(jax.random.fold_in(key, 13), -4.0, 4.0, (PACK_TOKENS, KEY_VALUE_HEADS * HEAD_SIZE), jnp.float32)
    return picked_rows.astype(jnp.bfloat16)


def draw_queries(key, part):
    picked_rows = jax.random.truncated_normal(jax.random.fold_in(key, 14), -4.0, 4.0, (PACK_TOKENS, QUERY_HEADS * HEAD_SIZE), jnp.float32)
    return picked_rows.astype(jnp.bfloat16)


def level_of(own_key, dims, pieces, smallest, top_value):
    factor_of, own = 1.0, jax.random.fold_in(own_key, 6)
    for dim, blocks in pieces:
        heights = jnp.exp(jax.random.uniform(jax.random.fold_in(own, dim), (blocks,), jnp.float32, smallest / len(pieces), top_value / len(pieces)))
        factor_of = factor_of * jnp.repeat(heights, dims[dim] // blocks).reshape([-1 if axis == dim else 1 for axis in range(len(dims))])
    return factor_of


def split_up(count, total, most, slope):
    weights = [(1 << 20) // math.isqrt(standing ** slope) + 1 for standing in range(2, count + 1)]
    surplus, counts = total - most - (count - 1), [1] * (count - 1)
    while surplus > 0:
        movable = [i for i in range(count - 1) if counts[i] < most]
        mass, remaining = sum([weights[i] for i in movable]), surplus
        for i in movable:
            extra = min(most - counts[i], max(1, remaining * weights[i] // mass), surplus)
            counts[i] = counts[i] + extra
            surplus = surplus - extra
    return np.array([most] + counts)


def uneven_parts(stream_key, amount, total, reach, lean):
    if amount == 2:
        one = jax.random.randint(stream_key, (), max(1, total - reach), min(reach, total - 1) + 1)
        return jnp.stack([one, total - one])
    tallies = jnp.asarray(split_up(amount, total, reach, lean), jnp.int32)
    pairs = (amount - 1) // 2
    giver, sink = tallies[1:1 + 2 * pairs:2], tallies[2:2 + 2 * pairs:2]
    margin = jnp.minimum(giver - 1, reach - sink)
    passed = jax.random.randint(jax.random.fold_in(stream_key, 1), (pairs,), 0, 1 << 20) % (margin + 1)
    tallies = tallies.at[1:1 + 2 * pairs:2].set(giver - passed).at[2:2 + 2 * pairs:2].set(sink + passed)
    return tallies[jax.random.permutation(jax.random.fold_in(stream_key, 2), amount)]


def scatter_about(rng, shape, scale, bound, shards=(), kind=jnp.bfloat16):
    level = level_of(rng, shape, shards, -0.22, 0.18) if shards else 1.0
    values = jax.random.normal(rng, shape, jnp.float32) * scale * level
    return jnp.minimum(jnp.maximum(values, -bound), bound).astype(kind)


def setup_inputs(seed: int = 0) -> dict:
    arg_keys = jax.random.split(jax.random.key(seed), 7)
    queries = draw_queries(jax.random.fold_in(arg_keys[6], 71), 0)
    keys = draw_keys(jax.random.fold_in(arg_keys[6], 71), 0)
    values = scatter_about(arg_keys[2], (PACK_TOKENS, KEY_VALUE_HEADS * HEAD_SIZE), 1.0, 6.0, ((0, 64), (1, 4)))
    doc_blocks = uneven_parts(arg_keys[3], NDOC, NBLK, MOSTB, 2).astype(jnp.int32)
    block_order = jax.random.permutation(arg_keys[4], NBLK).astype(jnp.int32)
    out_weight = scatter_about(arg_keys[5], (QUERY_HEADS * HEAD_SIZE, WIN), HEAD_SIZE ** -0.5, 0.5, ((0, 4),))
    return dict(queries=queries, keys=keys, values=values, doc_blocks=doc_blocks, block_order=block_order, out_weight=out_weight)


document_masked_score = -1.0e30


def reference(queries, keys, values, doc_blocks, block_order, out_weight):
    token_blocks = PACK_TOKENS // BLOCK_TOKENS
    block_ids = jnp.arange(token_blocks, dtype=jnp.int32)
    inverse_order = jnp.zeros((token_blocks,), jnp.int32).at[block_order].set(block_ids)
    sequence_queries = queries.reshape(token_blocks, BLOCK_TOKENS, KEY_VALUE_HEADS, GROUP_HEADS, HEAD_SIZE)[inverse_order]
    sequence_keys = keys.reshape(token_blocks, BLOCK_TOKENS, KEY_VALUE_HEADS, HEAD_SIZE)[inverse_order]
    sequence_values = values.reshape(token_blocks, BLOCK_TOKENS, KEY_VALUE_HEADS, HEAD_SIZE)[inverse_order]
    doc_ends = jnp.cumsum(doc_blocks).astype(jnp.int32)
    doc_of = jnp.sum((block_ids[:, None] >= doc_ends[None, :]).astype(jnp.int32), axis=1)
    doc_first = (doc_ends - doc_blocks).astype(jnp.int32)[doc_of]
    inner = jnp.arange(BLOCK_TOKENS, dtype=jnp.int32)

    def one_block(seq_block):
        query_rows = sequence_queries[seq_block].astype(jnp.float32)

        def add_tile(key_block, online):
            running_max, weight_sum, weighted = online
            key_rows = sequence_keys[key_block].astype(jnp.float32)
            value_rows = sequence_values[key_block].astype(jnp.float32)
            scores = jnp.einsum('qhgd,khd->hgqk', query_rows, key_rows) * (HEAD_SIZE ** -0.5)
            allowed = (key_block * BLOCK_TOKENS + inner[None, :]) <= (seq_block * BLOCK_TOKENS + inner[:, None])
            scores = jnp.where(allowed, scores, document_masked_score)
            new_max = jnp.maximum(running_max, jnp.max(scores, axis=-1))
            weights = jnp.where(allowed, jnp.exp(scores - new_max[..., None]), 0.0)
            factor = jnp.exp(running_max - new_max)
            weight_sum = weight_sum * factor + jnp.sum(weights, axis=-1)
            rounded = lax.optimization_barrier(weights.astype(jnp.bfloat16)).astype(jnp.float32)
            weighted = weighted * factor[..., None] + jnp.einsum('hgqk,khd->hgqd', rounded, value_rows)
            return new_max, weight_sum, weighted

        starting_state = (jnp.full((KEY_VALUE_HEADS, GROUP_HEADS, BLOCK_TOKENS), document_masked_score, jnp.float32),
                   jnp.zeros((KEY_VALUE_HEADS, GROUP_HEADS, BLOCK_TOKENS), jnp.float32),
                   jnp.zeros((KEY_VALUE_HEADS, GROUP_HEADS, BLOCK_TOKENS, HEAD_SIZE), jnp.float32))
        running_max, weight_sum, weighted = lax.fori_loop(doc_first[seq_block], seq_block + 1, add_tile, starting_state)
        result = weighted / weight_sum[..., None]
        return jnp.transpose(result, (2, 0, 1, 3)).reshape(BLOCK_TOKENS, QUERY_HEADS * HEAD_SIZE).astype(jnp.bfloat16)

    attended_seq = lax.map(one_block, block_ids)
    attended = attended_seq[block_order].reshape(PACK_TOKENS, QUERY_HEADS * HEAD_SIZE)
    return jnp.dot(attended, out_weight, preferred_element_type=jnp.float32).astype(jnp.bfloat16)
```

```python
import functools
import math

import jax
import jax.numpy as jnp
from jax import lax
from jax.experimental import pallas as pl
from jax.experimental.pallas import tpu as pltpu
from jax.sharding import PartitionSpec as P

BF16, F32 = jnp.bfloat16, jnp.float32
Z, X, TP = 8, 4, 4
ROWS, HEAD, HKV, GROUP = 128, 128, 2, 8
QL = GROUP * ROWS
WIN = 4096
TILE = 256
NCHUNK, COLS = 8, 512
ONES = 16
FAR = 1e30
SCALE = HEAD**-0.5 * math.log2(math.e)
DELTA = (0, -1, 1, 2)
MESH_ID = pl.DeviceIdType.MESH

ORDER = (
    ((0, 0), (1, 0), (0, -1), (1, -1), (0, 1), (1, 1), (1, -2), (0, -2), (1, 2), (0, 2), (1, -3), (1, 3), (0, -3), (1, 4), (0, 3), (0, 4)),
    ((1, 0), (0, 0), (1, -1), (0, -1), (1, 1), (0, 1), (1, -2), (1, 2), (0, -2), (0, 2), (1, -3), (1, 3), (0, -3), (0, 3), (1, 4), (0, 4)),
)


def events():
    both, k, v = "b", "k", "v"
    zero = [[] for _ in range(16)]
    zero[0] += [
        ((0, -1), (both,), [(k, "x+"), (both, "z+"), (both, "z-"), (both, "s")]),
        ((0, 1), (both,), [(v, "x-"), (both, "z+"), (both, "z-"), (both, "s")]),
    ]
    zero[1] += [((0, 2), (k, v), [(both, "z+"), (both, "z-"), (both, "s")])]
    for step in range(1, 4):
        for j in range(4):
            zero[4 * (step - 1) + j] += [
                ((-step, DELTA[j]), (both,), [(k if step == 3 else both, "z+"), (both, "s")]),
                ((step, DELTA[j]), (both,), [(v if step == 3 else both, "z-"), (both, "s")]),
            ]
    for j in range(4):
        zero[12 + j] += [((4, DELTA[j]), (k, v), [(both, "s")])]

    def along_z(step):
        if step == 4:
            return [((4, 0), (k, v), [(both, "x+"), (both, "x-"), (both, "s")])]
        return [
            ((-step, 0), (both,), [(k if step == 3 else both, "z+"), (both, "x+"), (both, "x-"), (both, "s")]),
            ((step, 0), (both,), [(v if step == 3 else both, "z-"), (both, "x+"), (both, "x-"), (both, "s")]),
        ]

    def near(dz):
        return [((dz, -1), (both,), [(k, "x+"), (both, "s")]), ((dz, 1), (both,), [(v, "x-"), (both, "s")])]

    def across(dz):
        return [((dz, 2), (k, v), [(both, "s")])]

    one = [
        near(0) + along_z(1),
        across(0),
        along_z(2) + near(-1),
        near(1) + across(-1),
        across(1) + along_z(3),
        near(-2),
        near(2) + across(-2),
        across(2) + along_z(4),
        near(-3),
        near(3) + across(-3),
        across(3) + near(4),
        across(4),
        [],
        [],
        [],
        [],
    ]
    return zero, one


def kernel(
    q_ref, k_ref, v_ref, doc_ref, ord_ref, w_ref, out_ref,
    buf, qin, vin, wbuf, qt, acc, mx, att, part, rin, sums, left_in, right_in, outv,
    recv, recv2, send, y_send, y_recv, local, w_sem,
):
    cp, tp = lax.axis_index("cp"), lax.axis_index("tp")
    core, x, z = lax.rem(cp, 2), lax.rem(cp // 2, X), cp // (2 * X)

    def block_of(kind, dz, dx):
        return kind * Z + lax.rem(z + dz + Z, Z), lax.rem(x + dx + X, X)

    def at(to):
        if to == "s":
            return (cp + 1 - 2 * core, tp)
        dz, dx = {"z+": (1, 0), "z-": (-1, 0), "x+": (0, 1), "x-": (0, -1)}[to]
        return ((lax.rem(z + dz + Z, Z) * X + lax.rem(x + dx + X, X)) * 2 + core, tp)

    def copy(group, col, piece, target, index):
        if piece == "b":
            ref, sem = buf.at[group, col], recv.at[group * X + col]
        elif piece == "k":
            ref, sem = buf.at[group, col, 0], recv.at[group * X + col]
        else:
            ref, sem = buf.at[group, col, 1], recv2.at[group * X + col]
        return pltpu.make_async_remote_copy(
            src_ref=ref, dst_ref=ref, send_sem=send.at[index], recv_sem=sem,
            device_id=target, device_id_type=MESH_ID,
        )

    my_group, my_col = core * Z + z, x
    neighbours = [at(to) for to in ("s", "z+", "z-", "x+", "x-")]
    up, down = (cp, lax.rem(tp + 1, TP)), (cp, lax.rem(tp + TP - 1, TP))
    neighbours += [up, down]

    loads = [
        pltpu.make_async_copy(v_ref, vin, local.at[0]),
        pltpu.make_async_copy(k_ref.at[:, 0:HEAD], buf.at[my_group, my_col, 0, 0], local.at[1]),
        pltpu.make_async_copy(k_ref.at[:, HEAD : 2 * HEAD], buf.at[my_group, my_col, 0, 1], local.at[2]),
        pltpu.make_async_copy(q_ref, qin, local.at[3]),
    ]
    for c in loads:
        c.start()
    weights = [
        pltpu.make_async_copy(
            w_ref.at[:, n * COLS : (n + 1) * COLS], wbuf.at[:, n * COLS : (n + 1) * COLS], w_sem.at[n]
        )
        for n in range(NCHUNK)
    ]
    barrier = pltpu.get_barrier_semaphore()
    for device in neighbours:
        pl.semaphore_signal(barrier, inc=1, device_id=device, device_id_type=MESH_ID)
    loads[0].wait()
    for h in range(HKV):
        vt = vin[:, h * HEAD : (h + 1) * HEAD].astype(F32).T.astype(BF16)
        buf[my_group, my_col, 1, h] = vt
    loads[1].wait()
    loads[2].wait()
    pl.semaphore_wait(barrier, len(neighbours))

    own_to = ("z+", "z-", "x+", "x-", "s")
    for i, to in enumerate(own_to):
        copy(my_group, my_col, "b", at(to), i).start()
    for c in weights:
        c.start()

    loads[3].wait()
    for h in range(HKV):
        for g in range(GROUP):
            i = h * GROUP + g
            scaled = (qin[:, i * HEAD : (i + 1) * HEAD].astype(F32) * SCALE).T
            high = scaled.astype(BF16)
            qt[h, 0:HEAD, g * ROWS : (g + 1) * ROWS] = high
            qt[h, HEAD : 2 * HEAD, g * ROWS : (g + 1) * ROWS] = (scaled - high.astype(F32)).astype(BF16)

    own_seq = ord_ref[cp]
    first_seq, end = jnp.int32(0), jnp.int32(0)
    for d in range(4):
        end = end + doc_ref[d]
        first_seq = jnp.where(end <= own_seq, end, first_seq)

    tiles = [(h, i) for h in range(HKV) for i in range(QL // TILE)]

    key_at = lax.broadcasted_iota(jnp.int32, (ROWS, TILE), 0)
    query_at = lax.rem(lax.broadcasted_iota(jnp.int32, (ROWS, TILE), 1), ROWS)
    seen = key_at <= query_at
    ones = jnp.ones((ONES, ROWS), BF16)
    for h, i in tiles:
        lanes = slice(i * TILE, (i + 1) * TILE)
        keys = buf[my_group, my_col, 0, h]
        s = jnp.dot(jnp.concatenate([keys, keys], axis=1), qt[h, :, lanes], preferred_element_type=F32)
        s = jnp.where(seen, s, -FAR)
        m = jnp.max(s, axis=0, keepdims=True)
        p = jnp.exp2(s - m).astype(BF16)
        values = jnp.concatenate([buf[my_group, my_col, 1, h], ones], axis=0)
        acc[h, :, lanes] = jnp.dot(values, p, preferred_element_type=F32)
        mx[h, :, lanes] = m

    plans = events()
    sends = ([(p, i) for i, p in enumerate("bbbbb")], [(p, i) for i, p in enumerate("bbbbb")])
    by_step = []
    for kind in range(2):
        index, steps = len(own_to), []
        for step in plans[kind]:
            now = []
            for where, waits, to in step:
                outs = []
                for piece, target in to:
                    outs.append((piece, target, index))
                    sends[kind].append((piece, index))
                    index += 1
                now.append((where, waits, outs))
            steps.append(now)
        by_step.append(steps)

    def communicate(t, kind):
        for (dz, dx), waits, outs in by_step[kind][t]:
            group, col = block_of(kind, dz, dx)
            for piece in waits:
                copy(group, col, piece, at("s"), 0).wait_recv()
            for piece, target, index in outs:
                copy(group, col, piece, at(target), index).start()

    def table(t, values):
        out = jnp.int32(values[0])
        for i in range(1, len(values)):
            out = jnp.where(t == i + 1, jnp.int32(values[i]), out)
        return out

    more_ones = jnp.ones((ONES, X * ROWS), BF16)

    def attend(group, biases):
        def scores(h, i):
            keys = buf[group, :, 0, h].reshape(X * ROWS, HEAD)
            return jnp.dot(
                jnp.concatenate([keys, keys], axis=1),
                qt[h, :, i * TILE : (i + 1) * TILE],
                preferred_element_type=F32,
            )

        coming = scores(*tiles[0])
        for n, (h, i) in enumerate(tiles):
            s = coming
            if n + 1 < len(tiles):
                coming = scores(*tiles[n + 1])
            lanes = slice(i * TILE, (i + 1) * TILE)
            blocks = [s[j * ROWS : (j + 1) * ROWS] for j in range(X)]
            old = mx[h, :, lanes]
            m = old
            for j in range(X):
                m = jnp.maximum(m, jnp.max(blocks[j], axis=0, keepdims=True) - biases[j])
            factor = jnp.exp2(old - m)
            p = jnp.concatenate([jnp.exp2(blocks[j] - (m + biases[j])).astype(BF16) for j in range(X)], axis=0)
            values = jnp.concatenate([buf[group, j, 1, h] for j in range(X)], axis=1)
            values = jnp.concatenate([values, more_ones], axis=0)
            acc[h, :, lanes] = acc[h, :, lanes] * factor + jnp.dot(values, p, preferred_element_type=F32)
            mx[h, :, lanes] = m

    for kind in range(2):

        @pl.when(core == kind)
        def _(kind=kind):
            communicate(0, kind)

    def step(t, carry):
        for i in range(1, 16):
            for kind in range(2):
                if by_step[kind][i]:

                    @pl.when((t == i) & (core == kind))
                    def _(i=i, kind=kind):
                        communicate(i, kind)

        kind = jnp.where(core == 0, table(t, [g for g, _ in ORDER[0]]), table(t, [g for g, _ in ORDER[1]]))
        away = jnp.where(core == 0, table(t, [d for _, d in ORDER[0]]), table(t, [d for _, d in ORDER[1]]))
        zz = lax.rem(z + away + Z, Z)
        group = kind * Z + zz

        @pl.when(kind != core)
        def _():
            for j in range(X):
                copy(group, j, "b", at("s"), 0).wait_recv()

        biases = []
        for j in range(X):
            seq = ord_ref[(zz * X + j) * 2 + kind]
            biases.append(jnp.where((seq >= first_seq) & (seq < own_seq), 0.0, FAR))
        attend(group, biases)
        return carry

    lax.fori_loop(1, 17, step, 0)

    for h in range(HKV):
        for g in range(GROUP):
            lanes = slice(g * ROWS, (g + 1) * ROWS)
            a = acc[h, 0:HEAD, lanes] / acc[h, HEAD : HEAD + 1, lanes]
            i = h * GROUP + g
            att[:, i * HEAD : (i + 1) * HEAD] = a.T.astype(BF16)

    own, above, below, over = tp, up[1], down[1], lax.rem(tp + 2, TP)
    half = NCHUNK // 2
    chunks = [n // 2 + (n % 2) * half for n in range(NCHUNK)]

    def y_copy(src, dst, index, target):
        return pltpu.make_async_remote_copy(
            src_ref=src, dst_ref=dst, send_sem=y_send.at[index], recv_sem=y_recv.at[index],
            device_id=target, device_id_type=MESH_ID,
        )

    def relay(n):
        return y_copy(part.at[n, over], rin.at[n], n, up if n < half else down)

    def direct(n):
        if n < half:
            return y_copy(part.at[n, below], right_in.at[n], NCHUNK + n, down)
        return y_copy(part.at[n, above], left_in.at[n], NCHUNK + n, up)

    def summed(n):
        if n < half:
            return y_copy(sums.at[n], left_in.at[n], 2 * NCHUNK + n, up)
        return y_copy(sums.at[n], right_in.at[n], 2 * NCHUNK + n, down)

    attended = att[...]
    ready = None
    for n in chunks:
        weights[n].wait()
        piece = jnp.dot(attended, wbuf[:, n * COLS : (n + 1) * COLS], preferred_element_type=F32)
        part[n] = piece.astype(BF16).reshape(TP, ROWS // TP, COLS)
        if ready is not None:
            relay(ready).start()
            direct(ready).start()
        ready = n
    relay(ready).start()
    direct(ready).start()
    ready = None
    for n in chunks:
        relay(n).wait_recv()
        onward = above if n < half else below
        sums[n] = (rin[n].astype(F32) + part[n, onward].astype(F32)).astype(BF16)
        if ready is not None:
            summed(ready).start()
        ready = n
    summed(ready).start()
    outs = []
    for n in chunks:
        direct(n).wait_recv()
        summed(n).wait_recv()
        total = part[n, own].astype(F32) + left_in[n].astype(F32) + right_in[n].astype(F32)
        outv[:, n * COLS : (n + 1) * COLS] = total.astype(BF16)
        outs.append(
            pltpu.make_async_copy(
                outv.at[:, n * COLS : (n + 1) * COLS], out_ref.at[:, n * COLS : (n + 1) * COLS], w_sem.at[n]
            )
        )
        outs[-1].start()

    for n in range(NCHUNK):
        relay(n).wait_send()
        direct(n).wait_send()
        summed(n).wait_send()
    for kind in range(2):

        @pl.when(core == kind)
        def _(kind=kind):
            for piece, index in sends[kind]:
                copy(my_group, my_col, piece, at("s"), index).wait_send()

    for c in outs:
        c.wait()


def local(queries, keys, values, doc_blocks, block_order, out_weight):
    any_, smem = pl.BlockSpec(memory_space=pl.ANY), pl.BlockSpec(memory_space=pltpu.SMEM)
    rows = ROWS // TP
    return pl.pallas_call(
        kernel,
        out_shape=jax.ShapeDtypeStruct((rows, WIN), BF16),
        in_specs=[any_, any_, any_, smem, smem, any_],
        out_specs=any_,
        scratch_shapes=[
            pltpu.VMEM((2 * Z, X, 2, HKV, ROWS, HEAD), BF16),
            pltpu.VMEM((ROWS, HKV * GROUP * HEAD), BF16),
            pltpu.VMEM((ROWS, HKV * HEAD), BF16),
            pltpu.VMEM((HKV * GROUP * HEAD, WIN), BF16),
            pltpu.VMEM((HKV, 2 * HEAD, QL), BF16),
            pltpu.VMEM((HKV, HEAD + ONES, QL), F32),
            pltpu.VMEM((HKV, 1, QL), F32),
            pltpu.VMEM((ROWS, HKV * GROUP * HEAD), BF16),
            pltpu.VMEM((NCHUNK, TP, rows, COLS), BF16),
            pltpu.VMEM((NCHUNK, rows, COLS), BF16),
            pltpu.VMEM((NCHUNK, rows, COLS), BF16),
            pltpu.VMEM((NCHUNK, rows, COLS), BF16),
            pltpu.VMEM((NCHUNK, rows, COLS), BF16),
            pltpu.VMEM((rows, WIN), BF16),
            pltpu.SemaphoreType.DMA((2 * Z * X,)),
            pltpu.SemaphoreType.DMA((2 * Z * X,)),
            pltpu.SemaphoreType.DMA((96,)),
            pltpu.SemaphoreType.DMA((3 * NCHUNK,)),
            pltpu.SemaphoreType.DMA((3 * NCHUNK,)),
            pltpu.SemaphoreType.DMA((4,)),
            pltpu.SemaphoreType.DMA((NCHUNK,)),
        ],
        compiler_params=pltpu.CompilerParams(
            collective_id=0, has_side_effects=True, vmem_limit_bytes=60 * 1024 * 1024
        ),
        name="attention",
    )(queries, keys, values, doc_blocks, block_order, out_weight)


def solution(mesh):
    placed = (P("cp", "tp"), P("cp", "tp"), P("cp", "tp"), P(), P(), P("tp", None))
    return jax.shard_map(
        local, mesh=mesh, in_specs=placed, out_specs=P(("cp", "tp"), None), check_vma=False
    )
```

```python
import functools
import math

import jax
import jax.numpy as jnp
from jax import lax
from jax.experimental import pallas as pl
from jax.experimental.pallas import tpu as pltpu
from jax.sharding import PartitionSpec as P

BF16, F32 = jnp.bfloat16, jnp.float32
Z, X, TP = 8, 4, 4
ROWS, HEAD, HKV, GROUP = 128, 128, 2, 8
QL = GROUP * ROWS
WIN = 4096
TILE = 256
NCHUNK, COLS = 8, 512
ONES = 16
FAR = 1e30
SCALE = HEAD**-0.5 * math.log2(math.e)
DELTA = (0, -1, 1, 2)
MESH_ID = pl.DeviceIdType.MESH

ORDER = (
    ((0, 0), (1, 0), (0, -1), (1, -1), (0, 1), (1, 1), (1, -2), (0, -2), (1, 2), (0, 2), (1, -3), (1, 3), (0, -3), (1, 4), (0, 3), (0, 4)),
    ((1, 0), (0, 0), (1, -1), (0, -1), (1, 1), (0, 1), (1, -2), (1, 2), (0, -2), (0, 2), (1, -3), (1, 3), (0, -3), (0, 3), (1, 4), (0, 4)),
)


def events():
    both, k, v = "b", "k", "v"
    zero = [[] for _ in range(16)]
    zero[0] += [
        ((0, -1), (both,), [(k, "x+"), (both, "z+"), (both, "z-"), (both, "s")]),
        ((0, 1), (both,), [(v, "x-"), (both, "z+"), (both, "z-"), (both, "s")]),
    ]
    zero[1] += [((0, 2), (k, v), [(both, "z+"), (both, "z-"), (both, "s")])]
    for step in range(1, 4):
        for j in range(4):
            zero[4 * (step - 1) + j] += [
                ((-step, DELTA[j]), (both,), [(k if step == 3 else both, "z+"), (both, "s")]),
                ((step, DELTA[j]), (both,), [(v if step == 3 else both, "z-"), (both, "s")]),
            ]
    for j in range(4):
        zero[12 + j] += [((4, DELTA[j]), (k, v), [(both, "s")])]

    def along_z(step):
        if step == 4:
            return [((4, 0), (k, v), [(both, "x+"), (both, "x-"), (both, "s")])]
        return [
            ((-step, 0), (both,), [(k if step == 3 else both, "z+"), (both, "x+"), (both, "x-"), (both, "s")]),
            ((step, 0), (both,), [(v if step == 3 else both, "z-"), (both, "x+"), (both, "x-"), (both, "s")]),
        ]

    def near(dz):
        return [((dz, -1), (both,), [(k, "x+"), (both, "s")]), ((dz, 1), (both,), [(v, "x-"), (both, "s")])]

    def across(dz):
        return [((dz, 2), (k, v), [(both, "s")])]

    one = [
        near(0) + along_z(1),
        across(0),
        along_z(2) + near(-1),
        near(1) + across(-1),
        across(1) + along_z(3),
        near(-2),
        near(2) + across(-2),
        across(2) + along_z(4),
        near(-3),
        near(3) + across(-3),
        across(3) + near(4),
        across(4),
        [],
        [],
        [],
        [],
    ]
    return zero, one


def kernel(
    q_ref, k_ref, v_ref, doc_ref, ord_ref, w_ref, out_ref,
    buf, qin, vin, wbuf, qt, acc, mx, att, part, rin, sums, left_in, right_in, outv,
    recv, recv2, send, y_send, y_recv, local, w_sem,
):
    cp, tp = lax.axis_index("cp"), lax.axis_index("tp")
    core, x, z = lax.rem(cp, 2), lax.rem(cp // 2, X), cp // (2 * X)

    def block_of(kind, dz, dx):
        return kind * Z + lax.rem(z + dz + Z, Z), lax.rem(x + dx + X, X)

    def at(to):
        if to == "s":
            return (cp + 1 - 2 * core, tp)
        dz, dx = {"z+": (1, 0), "z-": (-1, 0), "x+": (0, 1), "x-": (0, -1)}[to]
        return ((lax.rem(z + dz + Z, Z) * X + lax.rem(x + dx + X, X)) * 2 + core, tp)

    def copy(group, col, piece, target, index):
        if piece == "b":
            ref, sem = buf.at[group, col], recv.at[group * X + col]
        elif piece == "k":
            ref, sem = buf.at[group, col, 0], recv.at[group * X + col]
        else:
            ref, sem = buf.at[group, col, 1], recv2.at[group * X + col]
        return pltpu.make_async_remote_copy(
            src_ref=ref, dst_ref=ref, send_sem=send.at[index], recv_sem=sem,
            device_id=target, device_id_type=MESH_ID,
        )

    my_group, my_col = core * Z + z, x
    neighbours = [at(to) for to in ("s", "z+", "z-", "x+", "x-")]
    up, down = (cp, lax.rem(tp + 1, TP)), (cp, lax.rem(tp + TP - 1, TP))
    neighbours += [up, down]

    loads = [
        pltpu.make_async_copy(v_ref, vin, local.at[0]),
        pltpu.make_async_copy(k_ref.at[:, 0:HEAD], buf.at[my_group, my_col, 0, 0], local.at[1]),
        pltpu.make_async_copy(k_ref.at[:, HEAD : 2 * HEAD], buf.at[my_group, my_col, 0, 1], local.at[2]),
        pltpu.make_async_copy(q_ref, qin, local.at[3]),
    ]
    for c in loads:
        c.start()
    weights = [
        pltpu.make_async_copy(
            w_ref.at[:, n * COLS : (n + 1) * COLS], wbuf.at[:, n * COLS : (n + 1) * COLS], w_sem.at[n]
        )
        for n in range(NCHUNK)
    ]
    barrier = pltpu.get_barrier_semaphore()
    for device in neighbours:
        pl.semaphore_signal(barrier, inc=1, device_id=device, device_id_type=MESH_ID)
    with jax.named_scope("entry"):
        loads[0].wait()
        for h in range(HKV):
            vt = vin[:, h * HEAD : (h + 1) * HEAD].astype(F32).T.astype(BF16)
            buf[my_group, my_col, 1, h] = vt
        loads[1].wait()
        loads[2].wait()
        pl.semaphore_wait(barrier, len(neighbours))

    own_to = ("z+", "z-", "x+", "x-", "s")
    for i, to in enumerate(own_to):
        copy(my_group, my_col, "b", at(to), i).start()
    for c in weights:
        c.start()

    with jax.named_scope("queries"):
        loads[3].wait()
        for h in range(HKV):
            for g in range(GROUP):
                i = h * GROUP + g
                scaled = (qin[:, i * HEAD : (i + 1) * HEAD].astype(F32) * SCALE).T
                high = scaled.astype(BF16)
                qt[h, 0:HEAD, g * ROWS : (g + 1) * ROWS] = high
                qt[h, HEAD : 2 * HEAD, g * ROWS : (g + 1) * ROWS] = (scaled - high.astype(F32)).astype(BF16)

    own_seq = ord_ref[cp]
    first_seq, end = jnp.int32(0), jnp.int32(0)
    for d in range(4):
        end = end + doc_ref[d]
        first_seq = jnp.where(end <= own_seq, end, first_seq)

    tiles = [(h, i) for h in range(HKV) for i in range(QL // TILE)]

    key_at = lax.broadcasted_iota(jnp.int32, (ROWS, TILE), 0)
    query_at = lax.rem(lax.broadcasted_iota(jnp.int32, (ROWS, TILE), 1), ROWS)
    seen = key_at <= query_at
    ones = jnp.ones((ONES, ROWS), BF16)
    with jax.named_scope("own"):
        for h, i in tiles:
            lanes = slice(i * TILE, (i + 1) * TILE)
            keys = buf[my_group, my_col, 0, h]
            s = jnp.dot(jnp.concatenate([keys, keys], axis=1), qt[h, :, lanes], preferred_element_type=F32)
            s = jnp.where(seen, s, -FAR)
            m = jnp.max(s, axis=0, keepdims=True)
            p = jnp.exp2(s - m).astype(BF16)
            values = jnp.concatenate([buf[my_group, my_col, 1, h], ones], axis=0)
            acc[h, :, lanes] = jnp.dot(values, p, preferred_element_type=F32)
            mx[h, :, lanes] = m

    plans = events()
    sends = ([(p, i) for i, p in enumerate("bbbbb")], [(p, i) for i, p in enumerate("bbbbb")])
    by_step = []
    for kind in range(2):
        index, steps = len(own_to), []
        for step in plans[kind]:
            now = []
            for where, waits, to in step:
                outs = []
                for piece, target in to:
                    outs.append((piece, target, index))
                    sends[kind].append((piece, index))
                    index += 1
                now.append((where, waits, outs))
            steps.append(now)
        by_step.append(steps)

    def communicate(t, kind):
        for (dz, dx), waits, outs in by_step[kind][t]:
            group, col = block_of(kind, dz, dx)
            for piece in waits:
                copy(group, col, piece, at("s"), 0).wait_recv()
            for piece, target, index in outs:
                copy(group, col, piece, at(target), index).start()

    more_ones = jnp.ones((ONES, X * ROWS), BF16)

    def attend(group, biases):
        def scores(h, i):
            keys = buf[group, :, 0, h].reshape(X * ROWS, HEAD)
            return jnp.dot(
                jnp.concatenate([keys, keys], axis=1),
                qt[h, :, i * TILE : (i + 1) * TILE],
                preferred_element_type=F32,
            )

        coming = scores(*tiles[0])
        for n, (h, i) in enumerate(tiles):
            s = coming
            if n + 1 < len(tiles):
                coming = scores(*tiles[n + 1])
            lanes = slice(i * TILE, (i + 1) * TILE)
            blocks = [s[j * ROWS : (j + 1) * ROWS] for j in range(X)]
            old = mx[h, :, lanes]
            m = old
            for j in range(X):
                m = jnp.maximum(m, jnp.max(blocks[j], axis=0, keepdims=True) - biases[j])
            factor = jnp.exp2(old - m)
            p = jnp.concatenate([jnp.exp2(blocks[j] - (m + biases[j])).astype(BF16) for j in range(X)], axis=0)
            values = jnp.concatenate([buf[group, j, 1, h] for j in range(X)], axis=1)
            values = jnp.concatenate([values, more_ones], axis=0)
            acc[h, :, lanes] = acc[h, :, lanes] * factor + jnp.dot(values, p, preferred_element_type=F32)
            mx[h, :, lanes] = m

    for kind in range(2):

        @pl.when(core == kind)
        def _(kind=kind):
            with jax.named_scope("step0"):
                communicate(0, kind)

    def step(t, carry):
        def dispatch(kind, low, high):
            if high - low > 1:
                middle = (low + high) // 2
                return lax.cond(
                    t < middle, lambda: dispatch(kind, low, middle), lambda: dispatch(kind, middle, high)
                )
            if low < 16 and by_step[kind][low]:
                with jax.named_scope(f"step{low}"):
                    communicate(low, kind)
            of, away = ORDER[kind][low - 1]
            return jnp.int32(of), jnp.int32(away)

        kind, away = lax.cond(core == 0, lambda: dispatch(0, 1, 17), lambda: dispatch(1, 1, 17))
        zz = lax.rem(z + away + Z, Z)
        group = kind * Z + zz

        @pl.when(kind != core)
        def _():
            with jax.named_scope("sibling"):
                for j in range(X):
                    copy(group, j, "b", at("s"), 0).wait_recv()

        biases = []
        for j in range(X):
            seq = ord_ref[(zz * X + j) * 2 + kind]
            biases.append(jnp.where((seq >= first_seq) & (seq < own_seq), 0.0, FAR))
        with jax.named_scope("attend"):
            attend(group, biases)
        return carry

    lax.fori_loop(1, 17, step, 0)

    with jax.named_scope("attended"):
        for h in range(HKV):
            for g in range(GROUP):
                lanes = slice(g * ROWS, (g + 1) * ROWS)
                a = acc[h, 0:HEAD, lanes] / acc[h, HEAD : HEAD + 1, lanes]
                i = h * GROUP + g
                att[:, i * HEAD : (i + 1) * HEAD] = a.T.astype(BF16)

    own, above, below, over = tp, up[1], down[1], lax.rem(tp + 2, TP)
    half = NCHUNK // 2
    chunks = [n // 2 + (n % 2) * half for n in range(NCHUNK)]

    def y_copy(src, dst, index, target):
        return pltpu.make_async_remote_copy(
            src_ref=src, dst_ref=dst, send_sem=y_send.at[index], recv_sem=y_recv.at[index],
            device_id=target, device_id_type=MESH_ID,
        )

    def relay(n):
        return y_copy(part.at[n, over], rin.at[n], n, up if n < half else down)

    def direct(n):
        if n < half:
            return y_copy(part.at[n, below], right_in.at[n], NCHUNK + n, down)
        return y_copy(part.at[n, above], left_in.at[n], NCHUNK + n, up)

    def summed(n):
        if n < half:
            return y_copy(sums.at[n], left_in.at[n], 2 * NCHUNK + n, up)
        return y_copy(sums.at[n], right_in.at[n], 2 * NCHUNK + n, down)

    with jax.named_scope("project"):
        attended = att[...]
        ready = None
        for n in chunks:
            weights[n].wait()
            piece = jnp.dot(attended, wbuf[:, n * COLS : (n + 1) * COLS], preferred_element_type=F32)
            part[n] = piece.astype(BF16).reshape(TP, ROWS // TP, COLS)
            if ready is not None:
                relay(ready).start()
                direct(ready).start()
            ready = n
        relay(ready).start()
        direct(ready).start()
        ready = None
        for n in chunks:
            relay(n).wait_recv()
            onward = above if n < half else below
            sums[n] = (rin[n].astype(F32) + part[n, onward].astype(F32)).astype(BF16)
            if ready is not None:
                summed(ready).start()
            ready = n
        summed(ready).start()
        outs = []
        for n in chunks:
            direct(n).wait_recv()
            summed(n).wait_recv()
            total = part[n, own].astype(F32) + left_in[n].astype(F32) + right_in[n].astype(F32)
            outv[:, n * COLS : (n + 1) * COLS] = total.astype(BF16)
            outs.append(
                pltpu.make_async_copy(
                    outv.at[:, n * COLS : (n + 1) * COLS], out_ref.at[:, n * COLS : (n + 1) * COLS], w_sem.at[n]
                )
            )
            outs[-1].start()

    for n in range(NCHUNK):
        relay(n).wait_send()
        direct(n).wait_send()
        summed(n).wait_send()
    for kind in range(2):

        @pl.when(core == kind)
        def _(kind=kind):
            for piece, index in sends[kind]:
                copy(my_group, my_col, piece, at("s"), index).wait_send()

    for c in outs:
        c.wait()


def local(queries, keys, values, doc_blocks, block_order, out_weight):
    any_, smem = pl.BlockSpec(memory_space=pl.ANY), pl.BlockSpec(memory_space=pltpu.SMEM)
    rows = ROWS // TP
    return pl.pallas_call(
        kernel,
        out_shape=jax.ShapeDtypeStruct((rows, WIN), BF16),
        in_specs=[any_, any_, any_, smem, smem, any_],
        out_specs=any_,
        scratch_shapes=[
            pltpu.VMEM((2 * Z, X, 2, HKV, ROWS, HEAD), BF16),
            pltpu.VMEM((ROWS, HKV * GROUP * HEAD), BF16),
            pltpu.VMEM((ROWS, HKV * HEAD), BF16),
            pltpu.VMEM((HKV * GROUP * HEAD, WIN), BF16),
            pltpu.VMEM((HKV, 2 * HEAD, QL), BF16),
            pltpu.VMEM((HKV, HEAD + ONES, QL), F32),
            pltpu.VMEM((HKV, 1, QL), F32),
            pltpu.VMEM((ROWS, HKV * GROUP * HEAD), BF16),
            pltpu.VMEM((NCHUNK, TP, rows, COLS), BF16),
            pltpu.VMEM((NCHUNK, rows, COLS), BF16),
            pltpu.VMEM((NCHUNK, rows, COLS), BF16),
            pltpu.VMEM((NCHUNK, rows, COLS), BF16),
            pltpu.VMEM((NCHUNK, rows, COLS), BF16),
            pltpu.VMEM((rows, WIN), BF16),
            pltpu.SemaphoreType.DMA((2 * Z * X,)),
            pltpu.SemaphoreType.DMA((2 * Z * X,)),
            pltpu.SemaphoreType.DMA((96,)),
            pltpu.SemaphoreType.DMA((3 * NCHUNK,)),
            pltpu.SemaphoreType.DMA((3 * NCHUNK,)),
            pltpu.SemaphoreType.DMA((4,)),
            pltpu.SemaphoreType.DMA((NCHUNK,)),
        ],
        compiler_params=pltpu.CompilerParams(
            collective_id=0, has_side_effects=True, vmem_limit_bytes=60 * 1024 * 1024
        ),
        name="attention",
    )(queries, keys, values, doc_blocks, block_order, out_weight)


def solution(mesh):
    placed = (P("cp", "tp"), P("cp", "tp"), P("cp", "tp"), P(), P(), P("tp", None))
    return jax.shard_map(
        local, mesh=mesh, in_specs=placed, out_specs=P(("cp", "tp"), None), check_vma=False
    )
```

```python
import functools
import math

import jax
import jax.numpy as jnp
from jax import lax
from jax.experimental import pallas as pl
from jax.experimental.pallas import tpu as pltpu
from jax.sharding import PartitionSpec as P

BF16, F32 = jnp.bfloat16, jnp.float32
Z, X, TP = 8, 4, 4
ROWS, HEAD, HKV, GROUP = 128, 128, 2, 8
QL = GROUP * ROWS
WIN = 4096
TILE = 256
NCHUNK, COLS = 8, 512
ONES = 16
FAR = 1e30
SCALE = HEAD**-0.5 * math.log2(math.e)
MESH_ID = pl.DeviceIdType.MESH

PLAN = (
    (
        (((-1, 0), (1, 0), (0, -1), (0, 1)), ((1, 0, 0), (0, -1, 0), (0, 1, 0), (0, 0, 0))),
        ((), ((0, 0, -1), (0, 0, 1), (1, -1, 0), (1, 1, 0))),
        (((0, 2), (-2, 0), (2, 0)), ((1, 0, -1), (1, 0, 1), (0, 0, 2), (0, -2, 0))),
        (((-1, -1), (1, -1)), ((0, 2, 0), (1, -1, -1), (1, -1, 1), (0, -1, -1))),
        (((-1, 1), (1, 1)), ((0, 1, -1), (1, -2, 0), (1, 2, 0), (1, 1, -1))),
        ((), ((1, 1, 1), (0, -1, 1), (0, 1, 1), (1, 0, 2))),
        (((-1, 2), (1, 2)), ((1, -1, 2), (1, -2, -1), (1, -2, 1), (0, -1, 2))),
        (((-3, 0), (3, 0)), ((0, 1, 2), (1, -3, 0), (1, 3, 0), (1, 2, -1))),
        (((-2, -1), (2, -1)), ((1, 2, 1), (0, -3, 0), (0, 3, 0), (1, 1, 2))),
        (((-2, 1), (2, 1)), ((1, -2, 2), (0, -2, -1), (0, 2, -1), (0, -2, 1))),
        (((-2, 2), (2, 2)), ((0, 2, 1), (1, 4, 0), (1, -3, -1), (1, -3, 1))),
        (((4, 0),), ((0, -2, 2), (0, 2, 2), (1, 3, -1), (1, 3, 1))),
        (((-3, -1), (3, -1)), ((1, 2, 2), (0, 4, 0), (0, -3, -1), (0, 3, -1))),
        (((-3, 1), (3, 1)), ((1, 4, -1), (1, 4, 1), (1, -3, 2), (0, -3, 1))),
        (((-3, 2), (3, 2), (4, -1), (4, 1)), ((0, 3, 1), (1, 3, 2), (0, -3, 2), (0, 3, 2))),
        (((4, 2),), ((0, 4, -1), (0, 4, 1), (1, 4, 2), (0, 4, 2))),
    ),
    (
        (((-1, 0), (1, 0), (0, -1), (0, 1)), ((0, 0, 0), (1, -1, 0), (1, 1, 0), (1, 0, 0))),
        ((), ((1, 0, -1), (1, 0, 1), (0, -1, 0), (0, 1, 0))),
        (((-1, -1), (-1, 1)), ((0, 0, -1), (0, 0, 1), (1, -1, -1), (1, -1, 1))),
        (((-2, 0), (2, 0), (1, -1), (1, 1)), ((0, 0, 2), (1, -2, 0), (1, 2, 0), (1, 1, -1))),
        (((0, 2), (-1, 2)), ((1, 1, 1), (0, -2, 0), (0, 2, 0), (1, 0, 2))),
        (((-2, -1), (-2, 1)), ((1, -1, 2), (0, -1, -1), (0, 1, -1), (1, -2, -1))),
        (((-3, 0), (3, 0), (2, -1), (2, 1)), ((1, -2, 1), (0, -1, 1), (0, 1, 1), (1, -3, 0))),
        (((1, 2), (-2, 2)), ((1, 3, 0), (1, 2, -1), (1, 2, 1), (1, 1, 2))),
        ((), ((1, -2, 2), (0, -1, 2), (0, 1, 2), (0, -3, 0))),
        (((4, 0), (-3, -1), (-3, 1), (3, -1), (3, 1)), ((0, 3, 0), (0, -2, -1), (1, 4, 0), (1, -3, -1))),
        (((2, 2),), ((1, -3, 1), (1, 3, -1), (1, 3, 1), (0, 2, -1))),
        ((), ((0, -2, 1), (1, 2, 2), (0, 2, 1), (0, -2, 2))),
        (((4, -1), (4, 1), (-3, 2)), ((0, 2, 2), (0, 4, 0), (1, 4, -1), (1, 4, 1))),
        (((3, 2),), ((1, -3, 2), (0, -3, -1), (1, 3, 2), (0, 3, -1))),
        (((4, 2),), ((0, -3, 1), (0, 3, 1), (1, 4, 2), (0, -3, 2))),
        ((), ((0, 3, 2), (0, 4, -1), (0, 4, 1), (0, 4, 2))),
    ),
)


def routes(kind, dz, dx):
    z_way, z_piece = ("z+", "k") if dz < 0 else ("z-", "v")
    z_out = [("b" if abs(dz) < 3 else z_piece, z_way)] if 0 < abs(dz) < 4 else []
    turn = [("k", "x+")] if dx == -1 else [("v", "x-")] if dx == 1 else []
    wide = [("b", "x+"), ("b", "x-")]
    if dz == 0 and dx == 0:
        out = [("b", "z+"), ("b", "z-")] + wide
    elif kind == 0 and dz == 0:
        out = [("b", "z+"), ("b", "z-")] + turn
    elif kind == 0 and dz == 4:
        out = wide if dx == 0 else turn
    elif kind == 0:
        out = z_out if abs(dz) < 3 or dx == 0 else []
    else:
        out = z_out + wide if dx == 0 else turn
    return out + [("b", "s")]


def pieces(kind, dz, dx):
    if kind == 0:
        return "kv" if dx == 2 and dz in (0, 4) or (dz, dx) == (4, 0) else "b"
    return "kv" if dx == 2 or (dz, dx) == (4, 0) else "b"


def slot_of(kind, dz, dx):
    return (kind * Z + dz % Z) * X + dx % X


def second_sem(kind, dz, dx):
    if kind == 0:
        return {(0, 2): 0, (4, 0): 1, (4, 2): 2}[dz, dx]
    return 0 if dx == 0 else 1 + dz % Z


def kernel(
    q_ref, k_ref, v_ref, doc_ref, ord_ref, w_ref, out_ref,
    buf, qin, vin, wbuf, qt, acc, mx, att, part, rin, sums, left_in, right_in, outv,
    recv, recv2, send, y_send, y_recv, local, w_sem,
):
    cp, tp = lax.axis_index("cp"), lax.axis_index("tp")
    core, x, z = lax.rem(cp, 2), lax.rem(cp // 2, X), cp // (2 * X)

    def at(to):
        if to == "s":
            return (cp + 1 - 2 * core, tp)
        dz, dx = {"z+": (1, 0), "z-": (-1, 0), "x+": (0, 1), "x-": (0, -1)}[to]
        return ((lax.rem(z + dz + Z, Z) * X + lax.rem(x + dx + X, X)) * 2 + core, tp)

    def copy(kind, dz, dx, piece, to):
        mz, mx_ = {"s": (0, 0), "z+": (-1, 0), "z-": (1, 0), "x+": (0, -1), "x-": (0, 1)}[to]
        there = (kind, (dz + mz + 3) % Z - 3, (dx + mx_ + 1) % X - 1)
        here, dest = slot_of(kind, dz, dx), slot_of(*there)
        src, dst, sem = buf.at[here], buf.at[dest], recv.at[dest]
        if piece == "k":
            src, dst = buf.at[here, 0], buf.at[dest, 0]
        elif piece == "v":
            src, dst, sem = buf.at[here, 1], buf.at[dest, 1], recv2.at[second_sem(*there)]
        return pltpu.make_async_remote_copy(
            src_ref=src, dst_ref=dst, send_sem=send, recv_sem=sem, device_id=at(to), device_id_type=MESH_ID
        )

    def arrived(kind, dz, dx, how):
        slot = slot_of(kind, dz, dx)
        for piece in how:
            ref, sem = buf.at[slot], recv.at[slot]
            if piece == "k":
                ref = buf.at[slot, 0]
            elif piece == "v":
                ref, sem = buf.at[slot, 1], recv2.at[second_sem(kind, dz, dx)]
            pltpu.make_async_remote_copy(
                src_ref=ref, dst_ref=ref, send_sem=send, recv_sem=sem, device_id=at("s"), device_id_type=MESH_ID
            ).wait_recv()

    my_slot = core * (Z * X)
    neighbours = [at(to) for to in ("s", "z+", "z-", "x+", "x-")]
    up, down = (cp, lax.rem(tp + 1, TP)), (cp, lax.rem(tp + TP - 1, TP))
    neighbours += [up, down]

    loads = [
        pltpu.make_async_copy(v_ref, vin, local.at[0]),
        pltpu.make_async_copy(k_ref.at[:, 0:HEAD], buf.at[my_slot, 0, 0], local.at[1]),
        pltpu.make_async_copy(k_ref.at[:, HEAD : 2 * HEAD], buf.at[my_slot, 0, 1], local.at[2]),
        pltpu.make_async_copy(q_ref, qin, local.at[3]),
    ]
    for c in loads:
        c.start()
    weights = [
        pltpu.make_async_copy(
            w_ref.at[:, n * COLS : (n + 1) * COLS], wbuf.at[:, n * COLS : (n + 1) * COLS], w_sem.at[n]
        )
        for n in range(NCHUNK)
    ]
    barrier = pltpu.get_barrier_semaphore()
    for device in neighbours:
        pl.semaphore_signal(barrier, inc=1, device_id=device, device_id_type=MESH_ID)
    with jax.named_scope("entry"):
        loads[0].wait()
        for h in range(HKV):
            vt = vin[:, h * HEAD : (h + 1) * HEAD].astype(F32).T.astype(BF16)
            buf[my_slot, 1, h] = vt
        loads[1].wait()
        loads[2].wait()
        pl.semaphore_wait(barrier, len(neighbours))

    for kind in range(2):

        @pl.when(core == kind)
        def _(kind=kind):
            for piece, to in routes(kind, 0, 0):
                copy(kind, 0, 0, piece, to).start()

    for c in weights:
        c.start()

    with jax.named_scope("queries"):
        loads[3].wait()
        for h in range(HKV):
            for g in range(GROUP):
                i = h * GROUP + g
                scaled = (qin[:, i * HEAD : (i + 1) * HEAD].astype(F32) * SCALE).T
                high = scaled.astype(BF16)
                qt[h, 0:HEAD, g * ROWS : (g + 1) * ROWS] = high
                qt[h, HEAD : 2 * HEAD, g * ROWS : (g + 1) * ROWS] = (scaled - high.astype(F32)).astype(BF16)

    own_seq = ord_ref[cp]
    first_seq, end = jnp.int32(0), jnp.int32(0)
    for d in range(4):
        end = end + doc_ref[d]
        first_seq = jnp.where(end <= own_seq, end, first_seq)

    tiles = [(h, i) for h in range(HKV) for i in range(QL // TILE)]

    key_at = lax.broadcasted_iota(jnp.int32, (ROWS, TILE), 0)
    query_at = lax.rem(lax.broadcasted_iota(jnp.int32, (ROWS, TILE), 1), ROWS)
    seen = key_at <= query_at
    ones = jnp.ones((ONES, ROWS), BF16)
    with jax.named_scope("own"):
        for h, i in tiles:
            lanes = slice(i * TILE, (i + 1) * TILE)
            keys = buf[my_slot, 0, h]
            s = jnp.dot(jnp.concatenate([keys, keys], axis=1), qt[h, :, lanes], preferred_element_type=F32)
            s = jnp.where(seen, s, -FAR)
            m = jnp.max(s, axis=0, keepdims=True)
            p = jnp.exp2(s - m).astype(BF16)
            values = jnp.concatenate([buf[my_slot, 1, h], ones], axis=0)
            acc[h, :, lanes] = jnp.dot(values, p, preferred_element_type=F32)
            mx[h, :, lanes] = m

    more_ones = jnp.ones((ONES, X * ROWS), BF16)

    def attend(slots, biases):
        def scores(h, i):
            keys = jnp.concatenate([buf[slot, 0, h] for slot in slots], axis=0)
            return jnp.dot(
                jnp.concatenate([keys, keys], axis=1),
                qt[h, :, i * TILE : (i + 1) * TILE],
                preferred_element_type=F32,
            )

        coming = scores(*tiles[0])
        for n, (h, i) in enumerate(tiles):
            s = coming
            if n + 1 < len(tiles):
                coming = scores(*tiles[n + 1])
            lanes = slice(i * TILE, (i + 1) * TILE)
            blocks = [s[j * ROWS : (j + 1) * ROWS] for j in range(X)]
            old = mx[h, :, lanes]
            m = old
            for j in range(X):
                m = jnp.maximum(m, jnp.max(blocks[j], axis=0, keepdims=True) - biases[j])
            factor = jnp.exp2(old - m)
            p = jnp.concatenate([jnp.exp2(blocks[j] - (m + biases[j])).astype(BF16) for j in range(X)], axis=0)
            values = jnp.concatenate([buf[slot, 1, h] for slot in slots], axis=1)
            values = jnp.concatenate([values, more_ones], axis=0)
            acc[h, :, lanes] = acc[h, :, lanes] * factor + jnp.dot(values, p, preferred_element_type=F32)
            mx[h, :, lanes] = m

    def step(t, carry):
        def dispatch(kind, low, high):
            if high - low > 1:
                middle = (low + high) // 2
                return lax.cond(
                    t < middle, lambda: dispatch(kind, low, middle), lambda: dispatch(kind, middle, high)
                )
            passed, group = PLAN[kind][low]
            with jax.named_scope(f"step{low}"):
                for dz, dx in passed:
                    arrived(kind, dz, dx, pieces(kind, dz, dx))
                    for piece, to in routes(kind, dz, dx):
                        copy(kind, dz, dx, piece, to).start()
            with jax.named_scope(f"sib{low}"):
                for of, dz, dx in group:
                    if of != kind:
                        arrived(of, dz, dx, "b")
            return tuple(jnp.int32(slot_of(*block)) for block in group)

        slots = lax.cond(core == 0, lambda: dispatch(0, 0, 16), lambda: dispatch(1, 0, 16))
        biases = []
        for slot in slots:
            of, dz, dx = slot // (Z * X), lax.rem(slot // X, Z), lax.rem(slot, X)
            seq = ord_ref[(lax.rem(z + dz, Z) * X + lax.rem(x + dx, X)) * 2 + of]
            biases.append(jnp.where((seq >= first_seq) & (seq < own_seq), 0.0, FAR))
        with jax.named_scope("attend"):
            attend(slots, biases)
        return carry

    lax.fori_loop(0, 16, step, 0)

    with jax.named_scope("attended"):
        for h in range(HKV):
            for g in range(GROUP):
                lanes = slice(g * ROWS, (g + 1) * ROWS)
                a = acc[h, 0:HEAD, lanes] / acc[h, HEAD : HEAD + 1, lanes]
                i = h * GROUP + g
                att[:, i * HEAD : (i + 1) * HEAD] = a.T.astype(BF16)

    own, above, below, over = tp, up[1], down[1], lax.rem(tp + 2, TP)
    half = NCHUNK // 2
    chunks = [n // 2 + (n % 2) * half for n in range(NCHUNK)]

    def y_copy(src, dst, index, target):
        return pltpu.make_async_remote_copy(
            src_ref=src, dst_ref=dst, send_sem=y_send, recv_sem=y_recv.at[index],
            device_id=target, device_id_type=MESH_ID,
        )

    def relay(n):
        return y_copy(part.at[n, over], rin.at[n], n, up if n < half else down)

    def direct(n):
        if n < half:
            return y_copy(part.at[n, below], right_in.at[n], NCHUNK + n, down)
        return y_copy(part.at[n, above], left_in.at[n], NCHUNK + n, up)

    def summed(n):
        if n < half:
            return y_copy(sums.at[n], left_in.at[n], 2 * NCHUNK + n, up)
        return y_copy(sums.at[n], right_in.at[n], 2 * NCHUNK + n, down)

    with jax.named_scope("project"):
        attended = att[...]
        ready = None
        for n in chunks:
            weights[n].wait()
            piece = jnp.dot(attended, wbuf[:, n * COLS : (n + 1) * COLS], preferred_element_type=F32)
            part[n] = piece.astype(BF16).reshape(TP, ROWS // TP, COLS)
            if ready is not None:
                relay(ready).start()
                direct(ready).start()
            ready = n
        relay(ready).start()
        direct(ready).start()
        ready = None
        for n in chunks:
            relay(n).wait_recv()
            onward = above if n < half else below
            sums[n] = (rin[n].astype(F32) + part[n, onward].astype(F32)).astype(BF16)
            if ready is not None:
                summed(ready).start()
            ready = n
        summed(ready).start()
        outs = []
        for n in chunks:
            direct(n).wait_recv()
            summed(n).wait_recv()
            total = part[n, own].astype(F32) + left_in[n].astype(F32) + right_in[n].astype(F32)
            outv[:, n * COLS : (n + 1) * COLS] = total.astype(BF16)
            outs.append(
                pltpu.make_async_copy(
                    outv.at[:, n * COLS : (n + 1) * COLS], out_ref.at[:, n * COLS : (n + 1) * COLS], w_sem.at[n]
                )
            )
            outs[-1].start()

    sent = part.at[0 : 3 * NCHUNK // TP]
    y = pltpu.make_async_remote_copy(
        src_ref=sent, dst_ref=sent, send_sem=y_send, recv_sem=y_recv.at[0], device_id=up, device_id_type=MESH_ID
    )
    y.wait_send()
    sent = buf.at[0 : 2 * Z * X - 1]
    blocks = pltpu.make_async_remote_copy(
        src_ref=sent, dst_ref=sent, send_sem=send, recv_sem=recv.at[0], device_id=at("s"), device_id_type=MESH_ID
    )
    blocks.wait_send()
    for c in outs:
        c.wait()


def local(queries, keys, values, doc_blocks, block_order, out_weight):
    any_, smem = pl.BlockSpec(memory_space=pl.ANY), pl.BlockSpec(memory_space=pltpu.SMEM)
    rows = ROWS // TP
    return pl.pallas_call(
        kernel,
        out_shape=jax.ShapeDtypeStruct((rows, WIN), BF16),
        in_specs=[any_, any_, any_, smem, smem, any_],
        out_specs=any_,
        scratch_shapes=[
            pltpu.VMEM((2 * Z * X, 2, HKV, ROWS, HEAD), BF16),
            pltpu.VMEM((ROWS, HKV * GROUP * HEAD), BF16),
            pltpu.VMEM((ROWS, HKV * HEAD), BF16),
            pltpu.VMEM((HKV * GROUP * HEAD, WIN), BF16),
            pltpu.VMEM((HKV, 2 * HEAD, QL), BF16),
            pltpu.VMEM((HKV, HEAD + ONES, QL), F32),
            pltpu.VMEM((HKV, 1, QL), F32),
            pltpu.VMEM((ROWS, HKV * GROUP * HEAD), BF16),
            pltpu.VMEM((NCHUNK, TP, rows, COLS), BF16),
            pltpu.VMEM((NCHUNK, rows, COLS), BF16),
            pltpu.VMEM((NCHUNK, rows, COLS), BF16),
            pltpu.VMEM((NCHUNK, rows, COLS), BF16),
            pltpu.VMEM((NCHUNK, rows, COLS), BF16),
            pltpu.VMEM((rows, WIN), BF16),
            pltpu.SemaphoreType.DMA((2 * Z * X,)),
            pltpu.SemaphoreType.DMA((1 + Z,)),
            pltpu.SemaphoreType.DMA(()),
            pltpu.SemaphoreType.DMA(()),
            pltpu.SemaphoreType.DMA((3 * NCHUNK,)),
            pltpu.SemaphoreType.DMA((4,)),
            pltpu.SemaphoreType.DMA((NCHUNK,)),
        ],
        compiler_params=pltpu.CompilerParams(
            collective_id=0, has_side_effects=True, vmem_limit_bytes=60 * 1024 * 1024
        ),
        name="attention",
    )(queries, keys, values, doc_blocks, block_order, out_weight)


def solution(mesh):
    placed = (P("cp", "tp"), P("cp", "tp"), P("cp", "tp"), P(), P(), P("tp", None))
    return jax.shard_map(
        local, mesh=mesh, in_specs=placed, out_specs=P(("cp", "tp"), None), check_vma=False
    )
```

```python
import functools
import math

import jax
import jax.numpy as jnp
from jax import lax
from jax.experimental import pallas as pl
from jax.experimental.pallas import tpu as pltpu
from jax.sharding import PartitionSpec as P

BF16, F32 = jnp.bfloat16, jnp.float32
Z, X, TP = 8, 4, 4
ROWS, HEAD, HKV, GROUP = 128, 128, 2, 8
QL = GROUP * ROWS
WIN = 4096
TILE = 512
NCHUNK, COLS = 8, 512
ONES = 16
FAR = 1e30
SCALE = HEAD**-0.5 * math.log2(math.e)
MESH_ID = pl.DeviceIdType.MESH

PLAN = (
    (
        (((-1, 0), (1, 0), (0, -1), (0, 1)), ((1, 0, 0), (0, -1, 0), (0, 1, 0), (0, 0, 0))),
        ((), ((0, 0, -1), (0, 0, 1), (1, -1, 0), (1, 1, 0))),
        (((0, 2), (-2, 0), (2, 0)), ((1, 0, -1), (1, 0, 1), (0, 0, 2), (0, -2, 0))),
        (((-1, -1), (1, -1)), ((0, 2, 0), (1, -1, -1), (1, -1, 1), (0, -1, -1))),
        ((), ((0, 1, -1), (1, -2, 0), (1, 2, 0), (1, 1, -1))),
        (((-1, 1), (1, 1)), ((1, 1, 1), (1, 0, 2), (0, -1, 1), (0, 1, 1))),
        (((-1, 2), (1, 2)), ((1, -1, 2), (1, -2, -1), (1, -2, 1), (0, -1, 2))),
        ((), ((0, 1, 2), (1, -3, 0), (1, 3, 0), (1, 2, -1))),
        (((-3, 0), (3, 0)), ((1, 2, 1), (1, 1, 2), (0, -3, 0), (0, 3, 0))),
        (((-2, -1), (2, -1)), ((1, -2, 2), (0, -2, -1), (0, 2, -1), (1, 4, 0))),
        (((-2, 1), (2, 1)), ((1, -3, -1), (1, -3, 1), (0, -2, 1), (0, 2, 1))),
        (((-2, 2), (2, 2), (4, 0)), ((1, 3, -1), (0, -2, 2), (0, 2, 2), (0, 4, 0))),
        ((), ((1, 3, 1), (1, 2, 2), (1, 4, -1), (1, 4, 1))),
        (((-3, -1), (3, -1), (-3, 1), (3, 1)), ((1, -3, 2), (0, -3, -1), (0, 3, -1), (0, -3, 1))),
        (((-3, 2), (3, 2)), ((0, 3, 1), (1, 3, 2), (1, 4, 2), (0, -3, 2))),
        (((4, -1), (4, 1), (4, 2)), ((0, 3, 2), (0, 4, -1), (0, 4, 1), (0, 4, 2))),
    ),
    (
        (((-1, 0), (1, 0), (0, -1), (0, 1)), ((0, 0, 0), (1, -1, 0), (1, 1, 0), (1, 0, 0))),
        ((), ((1, 0, -1), (1, 0, 1), (0, -1, 0), (0, 1, 0))),
        (((-1, -1), (-1, 1)), ((0, 0, -1), (0, 0, 1), (1, -1, -1), (1, -1, 1))),
        (((-2, 0), (2, 0), (1, -1), (1, 1)), ((0, 0, 2), (1, -2, 0), (1, 2, 0), (1, 1, -1))),
        (((0, 2),), ((1, 1, 1), (0, -2, 0), (0, 2, 0), (1, 0, 2))),
        (((-1, 2), (-2, -1), (-2, 1)), ((0, -1, -1), (0, 1, -1), (1, -1, 2), (1, -2, -1))),
        (((-3, 0), (3, 0), (2, -1), (2, 1)), ((1, -2, 1), (0, -1, 1), (0, 1, 1), (1, -3, 0))),
        (((1, 2),), ((1, 3, 0), (1, 2, -1), (1, 2, 1), (1, 1, 2))),
        (((-2, 2), (4, 0), (-3, -1), (-3, 1)), ((0, -1, 2), (0, 1, 2), (1, -2, 2), (1, 4, 0))),
        ((), ((1, -3, -1), (1, -3, 1), (0, -3, 0), (0, 3, 0))),
        (((3, -1), (3, 1), (2, 2)), ((0, -2, -1), (0, 2, -1), (1, 3, -1), (1, 3, 1))),
        (((4, -1), (4, 1)), ((1, 2, 2), (0, -2, 1), (0, 2, 1), (1, 4, -1))),
        (((-3, 2),), ((1, 4, 1), (0, -2, 2), (0, 2, 2), (1, -3, 2))),
        (((3, 2), (4, 2)), ((0, 4, 0), (1, 3, 2), (1, 4, 2), (0, -3, -1))),
        ((), ((0, 3, -1), (0, -3, 1), (0, 3, 1), (0, -3, 2))),
        ((), ((0, 3, 2), (0, 4, -1), (0, 4, 1), (0, 4, 2))),
    ),
)


def routes(kind, dz, dx):
    z_way, z_piece = ("z+", "k") if dz < 0 else ("z-", "v")
    z_out = [("b" if abs(dz) < 3 else z_piece, z_way)] if 0 < abs(dz) < 4 else []
    turn = [("k", "x+")] if dx == -1 else [("v", "x-")] if dx == 1 else []
    wide = [("b", "x+"), ("b", "x-")]
    if dz == 0 and dx == 0:
        out = [("b", "z+"), ("b", "z-")] + wide
    elif kind == 0 and dz == 0:
        out = [("b", "z+"), ("b", "z-")] + turn
    elif kind == 0 and dz == 4:
        out = []
    elif kind == 0:
        out = z_out
    else:
        out = z_out + wide if dx == 0 else turn
    return out + [("b", "s")]


def pieces(kind, dz, dx):
    if kind == 0:
        return "kv" if dz == 4 or (dz, dx) == (0, 2) else "b"
    return "kv" if dx == 2 or (dz, dx) == (4, 0) else "b"


def slot_of(kind, dz, dx):
    return (kind * Z + dz % Z) * X + dx % X


def second_sem(kind, dz, dx):
    if kind == 0:
        return 4 if dz == 0 else dx % X
    return 0 if dx == 0 else 1 + dz % Z


def kernel(
    q_ref, k_ref, v_ref, doc_ref, ord_ref, w_ref, own_out, left_in, right_in,
    buf, qin, vin, wbuf, qt, acc, mx, att, part, rin, sums,
    recv, recv2, send, y_send, y_recv, local, w_sem,
):
    cp, tp = lax.axis_index("cp"), lax.axis_index("tp")
    core, x, z = lax.rem(cp, 2), lax.rem(cp // 2, X), cp // (2 * X)

    def at(to):
        if to == "s":
            return (cp + 1 - 2 * core, tp)
        dz, dx = {"z+": (1, 0), "z-": (-1, 0), "x+": (0, 1), "x-": (0, -1)}[to]
        return ((lax.rem(z + dz + Z, Z) * X + lax.rem(x + dx + X, X)) * 2 + core, tp)

    def copy(kind, dz, dx, piece, to):
        mz, mx_ = {"s": (0, 0), "z+": (-1, 0), "z-": (1, 0), "x+": (0, -1), "x-": (0, 1)}[to]
        there = (kind, (dz + mz + 3) % Z - 3, (dx + mx_ + 1) % X - 1)
        here, dest = slot_of(kind, dz, dx), slot_of(*there)
        src, dst, sem = buf.at[here], buf.at[dest], recv.at[dest]
        if piece == "k":
            src, dst = buf.at[here, 0], buf.at[dest, 0]
        elif piece == "v":
            src, dst, sem = buf.at[here, 1], buf.at[dest, 1], recv2.at[second_sem(*there)]
        return pltpu.make_async_remote_copy(
            src_ref=src, dst_ref=dst, send_sem=send, recv_sem=sem, device_id=at(to), device_id_type=MESH_ID
        )

    def arrived(kind, dz, dx, how):
        slot = slot_of(kind, dz, dx)
        for piece in how:
            ref, sem = buf.at[slot], recv.at[slot]
            if piece == "k":
                ref = buf.at[slot, 0]
            elif piece == "v":
                ref, sem = buf.at[slot, 1], recv2.at[second_sem(kind, dz, dx)]
            pltpu.make_async_remote_copy(
                src_ref=ref, dst_ref=ref, send_sem=send, recv_sem=sem, device_id=at("s"), device_id_type=MESH_ID
            ).wait_recv()

    my_slot = core * (Z * X)
    neighbours = [at(to) for to in ("s", "z+", "z-", "x+", "x-")]
    up, down = (cp, lax.rem(tp + 1, TP)), (cp, lax.rem(tp + TP - 1, TP))
    neighbours += [up, down]

    loads = [
        pltpu.make_async_copy(v_ref, vin, local.at[0]),
        pltpu.make_async_copy(k_ref.at[:, 0:HEAD], buf.at[my_slot, 0, 0], local.at[1]),
        pltpu.make_async_copy(k_ref.at[:, HEAD : 2 * HEAD], buf.at[my_slot, 0, 1], local.at[2]),
        pltpu.make_async_copy(q_ref, qin, local.at[3]),
    ]
    for c in loads:
        c.start()
    weights = [
        pltpu.make_async_copy(
            w_ref.at[:, n * COLS : (n + 1) * COLS], wbuf.at[:, n * COLS : (n + 1) * COLS], w_sem.at[n]
        )
        for n in range(NCHUNK)
    ]
    barrier = pltpu.get_barrier_semaphore()
    for device in neighbours:
        pl.semaphore_signal(barrier, inc=1, device_id=device, device_id_type=MESH_ID)
    with jax.named_scope("entry"):
        loads[0].wait()
        for h in range(HKV):
            vt = vin[:, h * HEAD : (h + 1) * HEAD].astype(F32).T.astype(BF16)
            buf[my_slot, 1, h] = vt
        loads[1].wait()
        loads[2].wait()
        pl.semaphore_wait(barrier, len(neighbours))

    for kind in range(2):

        @pl.when(core == kind)
        def _(kind=kind):
            for piece, to in routes(kind, 0, 0):
                copy(kind, 0, 0, piece, to).start()

    for c in weights:
        c.start()

    with jax.named_scope("queries"):
        loads[3].wait()
        for h in range(HKV):
            for g in range(GROUP):
                i = h * GROUP + g
                scaled = (qin[:, i * HEAD : (i + 1) * HEAD].astype(F32) * SCALE).T
                high = scaled.astype(BF16)
                qt[h, 0:HEAD, g * ROWS : (g + 1) * ROWS] = high
                qt[h, HEAD : 2 * HEAD, g * ROWS : (g + 1) * ROWS] = (scaled - high.astype(F32)).astype(BF16)

    own_seq = ord_ref[cp]
    first_seq, end = jnp.int32(0), jnp.int32(0)
    for d in range(4):
        end = end + doc_ref[d]
        first_seq = jnp.where(end <= own_seq, end, first_seq)

    tiles = [(h, i) for h in range(HKV) for i in range(QL // TILE)]

    key_at = lax.broadcasted_iota(jnp.int32, (ROWS, TILE), 0)
    query_at = lax.rem(lax.broadcasted_iota(jnp.int32, (ROWS, TILE), 1), ROWS)
    seen = key_at <= query_at
    ones = jnp.ones((ONES, ROWS), BF16)
    with jax.named_scope("own"):
        for h, i in tiles:
            lanes = slice(i * TILE, (i + 1) * TILE)
            keys = buf[my_slot, 0, h]
            s = jnp.dot(jnp.concatenate([keys, keys], axis=1), qt[h, :, lanes], preferred_element_type=F32)
            s = jnp.where(seen, s, -FAR)
            m = jnp.max(s, axis=0, keepdims=True)
            p = jnp.exp2(s - m).astype(BF16)
            values = jnp.concatenate([buf[my_slot, 1, h], ones], axis=0)
            acc[h, :, lanes] = jnp.dot(values, p, preferred_element_type=F32)
            mx[h, :, lanes] = m

    more_ones = jnp.ones((ONES, X * ROWS), BF16)

    def attend(slots, biases):
        def scores(h, i):
            keys = jnp.concatenate([buf[slot, 0, h] for slot in slots], axis=0)
            return jnp.dot(
                jnp.concatenate([keys, keys], axis=1),
                qt[h, :, i * TILE : (i + 1) * TILE],
                preferred_element_type=F32,
            )

        def soft(s, h, i):
            lanes = slice(i * TILE, (i + 1) * TILE)
            blocks = [s[j * ROWS : (j + 1) * ROWS] for j in range(X)]
            old = mx[h, :, lanes]
            m = old
            for j in range(X):
                m = jnp.maximum(m, jnp.max(blocks[j], axis=0, keepdims=True) - biases[j])
            mx[h, :, lanes] = m
            p = jnp.concatenate([jnp.exp2(blocks[j] - (m + biases[j])).astype(BF16) for j in range(X)], axis=0)
            return p, jnp.exp2(old - m)

        def add(p, factor, h, i):
            lanes = slice(i * TILE, (i + 1) * TILE)
            values = jnp.concatenate([buf[slot, 1, h] for slot in slots], axis=1)
            values = jnp.concatenate([values, more_ones], axis=0)
            acc[h, :, lanes] = acc[h, :, lanes] * factor + jnp.dot(values, p, preferred_element_type=F32)

        coming, waiting = scores(*tiles[0]), None
        for n, tile in enumerate(tiles):
            s = coming
            if n + 1 < len(tiles):
                coming = scores(*tiles[n + 1])
            if waiting is not None:
                add(*waiting)
            waiting = soft(s, *tile) + tile
        add(*waiting)

    def step(t, carry):
        def dispatch(kind, low, high):
            if high - low > 1:
                middle = (low + high) // 2
                return lax.cond(
                    t < middle, lambda: dispatch(kind, low, middle), lambda: dispatch(kind, middle, high)
                )
            passed, group = PLAN[kind][low]
            with jax.named_scope(f"step{low}"):
                for dz, dx in passed:
                    arrived(kind, dz, dx, pieces(kind, dz, dx))
                    for piece, to in routes(kind, dz, dx):
                        copy(kind, dz, dx, piece, to).start()
            with jax.named_scope(f"sib{low}"):
                for of, dz, dx in group:
                    if of != kind:
                        arrived(of, dz, dx, "b")
            return tuple(jnp.int32(slot_of(*block)) for block in group)

        slots = lax.cond(core == 0, lambda: dispatch(0, 0, 16), lambda: dispatch(1, 0, 16))
        biases = []
        for slot in slots:
            of, dz, dx = slot // (Z * X), lax.rem(slot // X, Z), lax.rem(slot, X)
            seq = ord_ref[(lax.rem(z + dz, Z) * X + lax.rem(x + dx, X)) * 2 + of]
            biases.append(jnp.where((seq >= first_seq) & (seq < own_seq), 0.0, FAR))
        with jax.named_scope("attend"):
            attend(slots, biases)
        return carry

    lax.fori_loop(0, 16, step, 0)

    with jax.named_scope("attended"):
        for h in range(HKV):
            for g in range(GROUP):
                lanes = slice(g * ROWS, (g + 1) * ROWS)
                a = acc[h, 0:HEAD, lanes] / acc[h, HEAD : HEAD + 1, lanes]
                i = h * GROUP + g
                att[:, i * HEAD : (i + 1) * HEAD] = a.T.astype(BF16)

    own, above, below, over = tp, up[1], down[1], lax.rem(tp + 2, TP)
    half = NCHUNK // 2
    chunks = [n // 2 + (n % 2) * half for n in range(NCHUNK)]

    def y_copy(src, dst, index, target):
        return pltpu.make_async_remote_copy(
            src_ref=src, dst_ref=dst, send_sem=y_send, recv_sem=y_recv.at[index],
            device_id=target, device_id_type=MESH_ID,
        )

    def cols(n):
        return slice(n * COLS, (n + 1) * COLS)

    def kept(n):
        return pltpu.make_async_copy(part.at[n, own], own_out.at[:, cols(n)], w_sem.at[n])

    def relay(n):
        return y_copy(part.at[n, over], rin.at[n], n, up if n < half else down)

    def direct(n):
        if n < half:
            return y_copy(part.at[n, below], right_in.at[:, cols(n)], NCHUNK + n, down)
        return y_copy(part.at[n, above], left_in.at[:, cols(n)], NCHUNK + n, up)

    def summed(n):
        if n < half:
            return y_copy(sums.at[n], left_in.at[:, cols(n)], 2 * NCHUNK + n, up)
        return y_copy(sums.at[n], right_in.at[:, cols(n)], 2 * NCHUNK + n, down)

    with jax.named_scope("project"):
        attended = att[...]
        ready = None
        for n in chunks:
            weights[n].wait()
            piece = jnp.dot(attended, wbuf[:, n * COLS : (n + 1) * COLS], preferred_element_type=F32)
            part[n] = piece.astype(BF16).reshape(TP, ROWS // TP, COLS)
            if ready is not None:
                relay(ready).start()
                direct(ready).start()
                kept(ready).start()
            ready = n
        relay(ready).start()
        direct(ready).start()
        kept(ready).start()
        ready = None
        for n in chunks:
            relay(n).wait_recv()
            onward = above if n < half else below
            sums[n] = (rin[n].astype(F32) + part[n, onward].astype(F32)).astype(BF16)
            if ready is not None:
                summed(ready).start()
            ready = n
        summed(ready).start()
        for n in chunks:
            direct(n).wait_recv()
            summed(n).wait_recv()

    sent = part.at[0 : 3 * NCHUNK // TP]
    y = pltpu.make_async_remote_copy(
        src_ref=sent, dst_ref=sent, send_sem=y_send, recv_sem=y_recv.at[0], device_id=up, device_id_type=MESH_ID
    )
    y.wait_send()
    sent = buf.at[0 : 2 * Z * X - 1]
    blocks = pltpu.make_async_remote_copy(
        src_ref=sent, dst_ref=sent, send_sem=send, recv_sem=recv.at[0], device_id=at("s"), device_id_type=MESH_ID
    )
    blocks.wait_send()
    for n in range(NCHUNK):
        kept(n).wait()


def local(queries, keys, values, doc_blocks, block_order, out_weight):
    any_, smem = pl.BlockSpec(memory_space=pl.ANY), pl.BlockSpec(memory_space=pltpu.SMEM)
    rows = ROWS // TP
    own, left, right = pl.pallas_call(
        kernel,
        out_shape=[jax.ShapeDtypeStruct((rows, WIN), BF16)] * 3,
        in_specs=[any_, any_, any_, smem, smem, any_],
        out_specs=[any_] * 3,
        scratch_shapes=[
            pltpu.VMEM((2 * Z * X, 2, HKV, ROWS, HEAD), BF16),
            pltpu.VMEM((ROWS, HKV * GROUP * HEAD), BF16),
            pltpu.VMEM((ROWS, HKV * HEAD), BF16),
            pltpu.VMEM((HKV * GROUP * HEAD, WIN), BF16),
            pltpu.VMEM((HKV, 2 * HEAD, QL), BF16),
            pltpu.VMEM((HKV, HEAD + ONES, QL), F32),
            pltpu.VMEM((HKV, 1, QL), F32),
            pltpu.VMEM((ROWS, HKV * GROUP * HEAD), BF16),
            pltpu.VMEM((NCHUNK, TP, rows, COLS), BF16),
            pltpu.VMEM((NCHUNK, rows, COLS), BF16),
            pltpu.VMEM((NCHUNK, rows, COLS), BF16),
            pltpu.SemaphoreType.DMA((2 * Z * X,)),
            pltpu.SemaphoreType.DMA((1 + Z,)),
            pltpu.SemaphoreType.DMA(()),
            pltpu.SemaphoreType.DMA(()),
            pltpu.SemaphoreType.DMA((3 * NCHUNK,)),
            pltpu.SemaphoreType.DMA((4,)),
            pltpu.SemaphoreType.DMA((NCHUNK,)),
        ],
        compiler_params=pltpu.CompilerParams(
            collective_id=0, has_side_effects=True, vmem_limit_bytes=60 * 1024 * 1024
        ),
        name="attention",
    )(queries, keys, values, doc_blocks, block_order, out_weight)
    return (own.astype(F32) + left.astype(F32) + right.astype(F32)).astype(BF16)


def solution(mesh):
    placed = (P("cp", "tp"), P("cp", "tp"), P("cp", "tp"), P(), P(), P("tp", None))
    return jax.shard_map(
        local, mesh=mesh, in_specs=placed, out_specs=P(("cp", "tp"), None), check_vma=False
    )
```

```python
import functools
import math

import jax
import jax.numpy as jnp
from jax import lax
from jax.experimental import pallas as pl
from jax.experimental.pallas import tpu as pltpu
from jax.sharding import PartitionSpec as P

BF16, F32 = jnp.bfloat16, jnp.float32
Z, X, TP = 8, 4, 4
ROWS, HEAD, HKV, GROUP = 128, 128, 2, 8
QL = GROUP * ROWS
WIN = 4096
TILE = 512
NCHUNK, COLS = 8, 512
ONES = 16
FAR = 1e30
SCALE = HEAD**-0.5 * math.log2(math.e)
MESH_ID = pl.DeviceIdType.MESH

PLAN = (
    (
        (((-1, 0), (1, 0), (0, -1), (0, 1)), ((1, 0, 0), (0, -1, 0), (0, 1, 0), (0, 0, 0))),
        ((), ((0, 0, -1), (0, 0, 1), (1, -1, 0), (1, 1, 0))),
        (((0, 2), (-2, 0), (2, 0)), ((1, 0, -1), (1, 0, 1), (0, 0, 2), (0, -2, 0))),
        (((-1, -1), (1, -1)), ((0, 2, 0), (1, -1, -1), (1, -1, 1), (0, -1, -1))),
        ((), ((0, 1, -1), (1, -2, 0), (1, 2, 0), (1, 1, -1))),
        (((-1, 1), (1, 1)), ((1, 1, 1), (1, 0, 2), (1, -1, 2), (0, -1, 1))),
        (((-1, 2), (1, 2)), ((0, 1, 1), (1, -2, -1), (1, -2, 1), (0, -1, 2))),
        (((-3, 0), (3, 0)), ((0, 1, 2), (1, -3, 0), (1, 3, 0), (0, -3, 0))),
        ((), ((0, 3, 0), (1, 2, -1), (1, 2, 1), (1, 1, 2))),
        (((-2, -1), (2, -1), (-2, 1), (2, 1)), ((1, -2, 2), (0, -2, -1), (0, 2, -1), (0, -2, 1))),
        (((-2, 2), (2, 2)), ((0, 2, 1), (1, 4, 0), (1, -3, -1), (1, -3, 1))),
        (((4, 0),), ((0, -2, 2), (0, 2, 2), (1, 3, -1), (1, 3, 1))),
        (((-3, -1), (3, -1)), ((1, 2, 2), (0, 4, 0), (1, 4, -1), (1, 4, 1))),
        (((-3, 1), (3, 1)), ((0, -3, -1), (0, 3, -1), (1, -3, 2), (0, -3, 1))),
        (((-3, 2), (3, 2)), ((0, 3, 1), (1, 3, 2), (1, 4, 2), (0, -3, 2))),
        (((4, -1), (4, 1), (4, 2)), ((0, 3, 2), (0, 4, -1), (0, 4, 1), (0, 4, 2))),
    ),
    (
        (((-1, 0), (1, 0), (0, -1), (0, 1)), ((0, 0, 0), (1, -1, 0), (1, 1, 0), (1, 0, 0))),
        ((), ((1, 0, -1), (1, 0, 1), (0, -1, 0), (0, 1, 0))),
        (((-1, -1), (-1, 1)), ((0, 0, -1), (0, 0, 1), (1, -1, -1), (1, -1, 1))),
        (((-2, 0), (2, 0), (1, -1), (1, 1)), ((0, 0, 2), (1, -2, 0), (1, 2, 0), (1, 1, -1))),
        (((0, 2), (-1, 2)), ((1, 1, 1), (0, -2, 0), (0, 2, 0), (1, 0, 2))),
        (((-2, -1), (-2, 1)), ((1, -1, 2), (0, -1, -1), (0, 1, -1), (1, -2, -1))),
        (((-3, 0), (3, 0), (2, -1), (2, 1)), ((1, -2, 1), (1, -3, 0), (1, 3, 0), (1, 2, -1))),
        (((1, 2), (-2, 2)), ((1, 2, 1), (0, -1, 1), (0, 1, 1), (1, 1, 2))),
        ((), ((1, -2, 2), (0, -1, 2), (0, 1, 2), (0, -3, 0))),
        (((4, 0), (-3, -1), (-3, 1)), ((0, 3, 0), (1, 4, 0), (1, -3, -1), (1, -3, 1))),
        (((3, -1), (3, 1), (2, 2)), ((0, -2, -1), (1, 3, -1), (1, 3, 1), (1, 2, 2))),
        (((4, -1), (4, 1)), ((0, 2, -1), (0, -2, 1), (0, 2, 1), (1, 4, -1))),
        (((-3, 2),), ((1, 4, 1), (0, -2, 2), (0, 2, 2), (1, -3, 2))),
        (((3, 2), (4, 2)), ((0, 4, 0), (1, 3, 2), (1, 4, 2), (0, -3, -1))),
        ((), ((0, 3, -1), (0, -3, 1), (0, 3, 1), (0, -3, 2))),
        ((), ((0, 3, 2), (0, 4, -1), (0, 4, 1), (0, 4, 2))),
    ),
)


def routes(kind, dz, dx):
    z_way, z_piece = ("z+", "k") if dz < 0 else ("z-", "v")
    z_out = [("b" if abs(dz) < 3 else z_piece, z_way)] if 0 < abs(dz) < 4 else []
    turn = [("k", "x+")] if dx == -1 else [("v", "x-")] if dx == 1 else []
    wide = [("b", "x+"), ("b", "x-")]
    if dz == 0 and dx == 0:
        out = [("b", "z+"), ("b", "z-")] + wide
    elif kind == 0 and dz == 0:
        out = [("b", "z+"), ("b", "z-")] + turn
    elif kind == 0 and dz == 4:
        out = []
    elif kind == 0:
        out = z_out
    else:
        out = z_out + wide if dx == 0 else turn
    return out + [("b", "s")]


def pieces(kind, dz, dx):
    if kind == 0:
        return "kv" if dz == 4 or (dz, dx) == (0, 2) else "b"
    return "kv" if dx == 2 or (dz, dx) == (4, 0) else "b"


def slot_of(kind, dz, dx):
    return (kind * Z + dz % Z) * X + dx % X


def second_sem(kind, dz, dx):
    if kind == 0:
        return 4 if dz == 0 else dx % X
    return 0 if dx == 0 else 1 + dz % Z


def kernel(
    q_ref, k_ref, v_ref, doc_ref, ord_ref, w_ref, own_out, left_in, right_in,
    buf, qin, vin, wbuf, qt, acc, mx, att, part, rin, sums,
    recv, recv2, send, y_send, y_recv, local, w_sem,
):
    cp, tp = lax.axis_index("cp"), lax.axis_index("tp")
    core, x, z = lax.rem(cp, 2), lax.rem(cp // 2, X), cp // (2 * X)

    def at(to):
        if to == "s":
            return (cp + 1 - 2 * core, tp)
        dz, dx = {"z+": (1, 0), "z-": (-1, 0), "x+": (0, 1), "x-": (0, -1)}[to]
        return ((lax.rem(z + dz + Z, Z) * X + lax.rem(x + dx + X, X)) * 2 + core, tp)

    def copy(kind, dz, dx, piece, to):
        mz, mx_ = {"s": (0, 0), "z+": (-1, 0), "z-": (1, 0), "x+": (0, -1), "x-": (0, 1)}[to]
        there = (kind, (dz + mz + 3) % Z - 3, (dx + mx_ + 1) % X - 1)
        here, dest = slot_of(kind, dz, dx), slot_of(*there)
        src, dst, sem = buf.at[here], buf.at[dest], recv.at[dest]
        if piece == "k":
            src, dst = buf.at[here, 0], buf.at[dest, 0]
        elif piece == "v":
            src, dst, sem = buf.at[here, 1], buf.at[dest, 1], recv2.at[second_sem(*there)]
        return pltpu.make_async_remote_copy(
            src_ref=src, dst_ref=dst, send_sem=send, recv_sem=sem, device_id=at(to), device_id_type=MESH_ID
        )

    def arrived(kind, dz, dx, how):
        slot = slot_of(kind, dz, dx)
        for piece in how:
            ref, sem = buf.at[slot], recv.at[slot]
            if piece == "k":
                ref = buf.at[slot, 0]
            elif piece == "v":
                ref, sem = buf.at[slot, 1], recv2.at[second_sem(kind, dz, dx)]
            pltpu.make_async_remote_copy(
                src_ref=ref, dst_ref=ref, send_sem=send, recv_sem=sem, device_id=at("s"), device_id_type=MESH_ID
            ).wait_recv()

    my_slot = core * (Z * X)
    neighbours = [at(to) for to in ("s", "z+", "z-", "x+", "x-")]
    up, down = (cp, lax.rem(tp + 1, TP)), (cp, lax.rem(tp + TP - 1, TP))
    neighbours += [up, down]

    loads = [
        pltpu.make_async_copy(v_ref, vin, local.at[0]),
        pltpu.make_async_copy(k_ref.at[:, 0:HEAD], buf.at[my_slot, 0, 0], local.at[1]),
        pltpu.make_async_copy(k_ref.at[:, HEAD : 2 * HEAD], buf.at[my_slot, 0, 1], local.at[2]),
        pltpu.make_async_copy(q_ref, qin, local.at[3]),
    ]
    for c in loads:
        c.start()
    weights = [
        pltpu.make_async_copy(
            w_ref.at[:, n * COLS : (n + 1) * COLS], wbuf.at[:, n * COLS : (n + 1) * COLS], w_sem.at[n]
        )
        for n in range(NCHUNK)
    ]
    barrier = pltpu.get_barrier_semaphore()
    for device in neighbours:
        pl.semaphore_signal(barrier, inc=1, device_id=device, device_id_type=MESH_ID)
    with jax.named_scope("entry"):
        loads[0].wait()
        for h in range(HKV):
            vt = vin[:, h * HEAD : (h + 1) * HEAD].astype(F32).T.astype(BF16)
            buf[my_slot, 1, h] = vt
        loads[1].wait()
        loads[2].wait()
        pl.semaphore_wait(barrier, len(neighbours))

    for kind in range(2):

        @pl.when(core == kind)
        def _(kind=kind):
            for piece, to in routes(kind, 0, 0):
                copy(kind, 0, 0, piece, to).start()

    for c in weights:
        c.start()

    with jax.named_scope("queries"):
        loads[3].wait()
        for h in range(HKV):
            for g in range(GROUP):
                i = h * GROUP + g
                scaled = (qin[:, i * HEAD : (i + 1) * HEAD].astype(F32) * SCALE).T
                high = scaled.astype(BF16)
                qt[h, 0:HEAD, g * ROWS : (g + 1) * ROWS] = high
                qt[h, HEAD : 2 * HEAD, g * ROWS : (g + 1) * ROWS] = (scaled - high.astype(F32)).astype(BF16)

    own_seq = ord_ref[cp]
    first_seq, end = jnp.int32(0), jnp.int32(0)
    for d in range(4):
        end = end + doc_ref[d]
        first_seq = jnp.where(end <= own_seq, end, first_seq)

    tiles = [(h, i) for h in range(HKV) for i in range(QL // TILE)]

    key_at = lax.broadcasted_iota(jnp.int32, (ROWS, TILE), 0)
    query_at = lax.rem(lax.broadcasted_iota(jnp.int32, (ROWS, TILE), 1), ROWS)
    seen = key_at <= query_at
    ones = jnp.ones((ONES, ROWS), BF16)
    with jax.named_scope("own"):
        for h, i in tiles:
            lanes = slice(i * TILE, (i + 1) * TILE)
            keys = buf[my_slot, 0, h]
            s = jnp.dot(jnp.concatenate([keys, keys], axis=1), qt[h, :, lanes], preferred_element_type=F32)
            s = jnp.where(seen, s, -FAR)
            m = jnp.max(s, axis=0, keepdims=True)
            p = jnp.exp2(s - m).astype(BF16)
            values = jnp.concatenate([buf[my_slot, 1, h], ones], axis=0)
            acc[h, :, lanes] = jnp.dot(values, p, preferred_element_type=F32)
            mx[h, :, lanes] = m

    more_ones = jnp.ones((ONES, X * ROWS), BF16)

    def attend(slots, biases):
        def scores(h, i):
            keys = jnp.concatenate([buf[slot, 0, h] for slot in slots], axis=0)
            return jnp.dot(
                jnp.concatenate([keys, keys], axis=1),
                qt[h, :, i * TILE : (i + 1) * TILE],
                preferred_element_type=F32,
            )

        def soft(s, h, i):
            lanes = slice(i * TILE, (i + 1) * TILE)
            blocks = [s[j * ROWS : (j + 1) * ROWS] for j in range(X)]
            old = mx[h, :, lanes]
            m = old
            for j in range(X):
                m = jnp.maximum(m, jnp.max(blocks[j], axis=0, keepdims=True) - biases[j])
            mx[h, :, lanes] = m
            p = jnp.concatenate([jnp.exp2(blocks[j] - (m + biases[j])).astype(BF16) for j in range(X)], axis=0)
            return p, jnp.exp2(old - m)

        def add(p, factor, h, i):
            lanes = slice(i * TILE, (i + 1) * TILE)
            values = jnp.concatenate([buf[slot, 1, h] for slot in slots], axis=1)
            values = jnp.concatenate([values, more_ones], axis=0)
            acc[h, :, lanes] = acc[h, :, lanes] * factor + jnp.dot(values, p, preferred_element_type=F32)

        coming, waiting = scores(*tiles[0]), None
        for n, tile in enumerate(tiles):
            s = coming
            if n + 1 < len(tiles):
                coming = scores(*tiles[n + 1])
            if waiting is not None:
                add(*waiting)
            waiting = soft(s, *tile) + tile
        add(*waiting)

    def step(t, carry):
        def dispatch(kind, low, high):
            if high - low > 1:
                middle = (low + high) // 2
                return lax.cond(
                    t < middle, lambda: dispatch(kind, low, middle), lambda: dispatch(kind, middle, high)
                )
            passed, group = PLAN[kind][low]
            with jax.named_scope(f"step{low}"):
                for dz, dx in passed:
                    arrived(kind, dz, dx, pieces(kind, dz, dx))
                    for piece, to in routes(kind, dz, dx):
                        copy(kind, dz, dx, piece, to).start()
            with jax.named_scope(f"sib{low}"):
                for of, dz, dx in group:
                    if of != kind:
                        arrived(of, dz, dx, "b")
            return tuple(jnp.int32(slot_of(*block)) for block in group)

        slots = lax.cond(core == 0, lambda: dispatch(0, 0, 16), lambda: dispatch(1, 0, 16))
        biases = []
        for slot in slots:
            of, dz, dx = slot // (Z * X), lax.rem(slot // X, Z), lax.rem(slot, X)
            seq = ord_ref[(lax.rem(z + dz, Z) * X + lax.rem(x + dx, X)) * 2 + of]
            biases.append(jnp.where((seq >= first_seq) & (seq < own_seq), 0.0, FAR))
        with jax.named_scope("attend"):
            attend(slots, biases)
        return carry

    lax.fori_loop(0, 16, step, 0)

    with jax.named_scope("attended"):
        for h in range(HKV):
            for g in range(GROUP):
                lanes = slice(g * ROWS, (g + 1) * ROWS)
                a = acc[h, 0:HEAD, lanes] / acc[h, HEAD : HEAD + 1, lanes]
                i = h * GROUP + g
                att[:, i * HEAD : (i + 1) * HEAD] = a.T.astype(BF16)

    own, above, below, over = tp, up[1], down[1], lax.rem(tp + 2, TP)
    half = NCHUNK // 2
    chunks = [n // 2 + (n % 2) * half for n in range(NCHUNK)]

    def y_copy(src, dst, index, target):
        return pltpu.make_async_remote_copy(
            src_ref=src, dst_ref=dst, send_sem=y_send, recv_sem=y_recv.at[index],
            device_id=target, device_id_type=MESH_ID,
        )

    def cols(n):
        return slice(n * COLS, (n + 1) * COLS)

    def kept(n):
        return pltpu.make_async_copy(part.at[n, own], own_out.at[:, cols(n)], w_sem.at[n])

    def relay(n):
        return y_copy(part.at[n, over], rin.at[n], n, up if n < half else down)

    def direct(n):
        if n < half:
            return y_copy(part.at[n, below], right_in.at[:, cols(n)], NCHUNK + n, down)
        return y_copy(part.at[n, above], left_in.at[:, cols(n)], NCHUNK + n, up)

    def summed(n):
        if n < half:
            return y_copy(sums.at[n], left_in.at[:, cols(n)], 2 * NCHUNK + n, up)
        return y_copy(sums.at[n], right_in.at[:, cols(n)], 2 * NCHUNK + n, down)

    with jax.named_scope("project"):
        attended = att[...]
        ready = None
        for n in chunks:
            weights[n].wait()
            piece = jnp.dot(attended, wbuf[:, n * COLS : (n + 1) * COLS], preferred_element_type=F32)
            part[n] = piece.astype(BF16).reshape(TP, ROWS // TP, COLS)
            if ready is not None:
                relay(ready).start()
                kept(ready).start()
            ready = n
        relay(ready).start()
        kept(ready).start()
        for n in chunks:
            direct(n).start()
        ready = None
        for n in chunks:
            relay(n).wait_recv()
            onward = above if n < half else below
            sums[n] = (rin[n].astype(F32) + part[n, onward].astype(F32)).astype(BF16)
            if ready is not None:
                summed(ready).start()
            ready = n
        summed(ready).start()
        for n in chunks:
            direct(n).wait_recv()
            summed(n).wait_recv()

    sent = part.at[0 : 3 * NCHUNK // TP]
    y = pltpu.make_async_remote_copy(
        src_ref=sent, dst_ref=sent, send_sem=y_send, recv_sem=y_recv.at[0], device_id=up, device_id_type=MESH_ID
    )
    y.wait_send()
    sent = buf.at[0 : 2 * Z * X - 1]
    blocks = pltpu.make_async_remote_copy(
        src_ref=sent, dst_ref=sent, send_sem=send, recv_sem=recv.at[0], device_id=at("s"), device_id_type=MESH_ID
    )
    blocks.wait_send()
    for n in range(NCHUNK):
        kept(n).wait()


def local(queries, keys, values, doc_blocks, block_order, out_weight):
    any_, smem = pl.BlockSpec(memory_space=pl.ANY), pl.BlockSpec(memory_space=pltpu.SMEM)
    rows = ROWS // TP
    own, left, right = pl.pallas_call(
        kernel,
        out_shape=[jax.ShapeDtypeStruct((rows, WIN), BF16)] * 3,
        in_specs=[any_, any_, any_, smem, smem, any_],
        out_specs=[any_] * 3,
        scratch_shapes=[
            pltpu.VMEM((2 * Z * X, 2, HKV, ROWS, HEAD), BF16),
            pltpu.VMEM((ROWS, HKV * GROUP * HEAD), BF16),
            pltpu.VMEM((ROWS, HKV * HEAD), BF16),
            pltpu.VMEM((HKV * GROUP * HEAD, WIN), BF16),
            pltpu.VMEM((HKV, 2 * HEAD, QL), BF16),
            pltpu.VMEM((HKV, HEAD + ONES, QL), F32),
            pltpu.VMEM((HKV, 1, QL), F32),
            pltpu.VMEM((ROWS, HKV * GROUP * HEAD), BF16),
            pltpu.VMEM((NCHUNK, TP, rows, COLS), BF16),
            pltpu.VMEM((NCHUNK, rows, COLS), BF16),
            pltpu.VMEM((NCHUNK, rows, COLS), BF16),
            pltpu.SemaphoreType.DMA((2 * Z * X,)),
            pltpu.SemaphoreType.DMA((1 + Z,)),
            pltpu.SemaphoreType.DMA(()),
            pltpu.SemaphoreType.DMA(()),
            pltpu.SemaphoreType.DMA((3 * NCHUNK,)),
            pltpu.SemaphoreType.DMA((4,)),
            pltpu.SemaphoreType.DMA((NCHUNK,)),
        ],
        compiler_params=pltpu.CompilerParams(
            collective_id=0, has_side_effects=True, vmem_limit_bytes=60 * 1024 * 1024
        ),
        name="attention",
    )(queries, keys, values, doc_blocks, block_order, out_weight)
    return (own.astype(F32) + left.astype(F32) + right.astype(F32)).astype(BF16)


def solution(mesh):
    placed = (P("cp", "tp"), P("cp", "tp"), P("cp", "tp"), P(), P(), P("tp", None))
    return jax.shard_map(
        local, mesh=mesh, in_specs=placed, out_specs=P(("cp", "tp"), None), check_vma=False
    )
```

```python
import functools
import math

import jax
import jax.numpy as jnp
from jax import lax
from jax.experimental import pallas as pl
from jax.experimental.pallas import tpu as pltpu
from jax.sharding import PartitionSpec as P

BF16, F32 = jnp.bfloat16, jnp.float32
Z, X, TP = 8, 4, 4
ROWS, HEAD, HKV, GROUP = 128, 128, 2, 8
QL = GROUP * ROWS
WIN = 4096
TILE = 512
NCHUNK, COLS = 8, 512
ONES = 16
FAR = 1e30
SCALE = HEAD**-0.5 * math.log2(math.e)
MESH_ID = pl.DeviceIdType.MESH

PLAN = (
    (
        (((-1, 0), (1, 0), (0, -1), (0, 1)), ((1, 0, 0), (0, -1, 0), (0, 1, 0), (0, 0, 0))),
        ((), ((0, 0, -1), (0, 0, 1), (1, -1, 0), (1, 1, 0))),
        (((0, 2), (-2, 0), (2, 0)), ((1, 0, -1), (1, 0, 1), (0, 0, 2), (0, -2, 0))),
        (((-1, -1), (1, -1)), ((0, 2, 0), (1, -1, -1), (1, -1, 1), (0, -1, -1))),
        ((), ((0, 1, -1), (1, -2, 0), (1, 2, 0), (1, 1, -1))),
        (((-1, 1), (1, 1)), ((1, 1, 1), (1, 0, 2), (0, -1, 1), (0, 1, 1))),
        (((-1, 2), (1, 2)), ((1, -1, 2), (1, -2, -1), (1, -2, 1), (0, -1, 2))),
        ((), ((0, 1, 2), (1, -3, 0), (1, 3, 0), (1, 2, -1))),
        (((-3, 0), (3, 0)), ((1, 2, 1), (1, 1, 2), (0, -3, 0), (0, 3, 0))),
        (((-2, -1), (2, -1)), ((1, -2, 2), (0, -2, -1), (0, 2, -1), (1, 4, 0))),
        (((-2, 1), (2, 1)), ((1, -3, -1), (1, -3, 1), (0, -2, 1), (0, 2, 1))),
        (((-2, 2), (2, 2), (4, 0)), ((1, 3, -1), (0, -2, 2), (0, 2, 2), (0, 4, 0))),
        ((), ((1, 3, 1), (1, 2, 2), (1, 4, -1), (1, 4, 1))),
        (((-3, -1), (3, -1), (-3, 1), (3, 1)), ((1, -3, 2), (0, -3, -1), (0, 3, -1), (0, -3, 1))),
        (((-3, 2), (3, 2)), ((0, 3, 1), (1, 3, 2), (1, 4, 2), (0, -3, 2))),
        (((4, -1), (4, 1), (4, 2)), ((0, 3, 2), (0, 4, -1), (0, 4, 1), (0, 4, 2))),
    ),
    (
        (((-1, 0), (1, 0), (0, -1), (0, 1)), ((0, 0, 0), (1, -1, 0), (1, 1, 0), (1, 0, 0))),
        ((), ((1, 0, -1), (1, 0, 1), (0, -1, 0), (0, 1, 0))),
        (((-1, -1), (-1, 1)), ((0, 0, -1), (0, 0, 1), (1, -1, -1), (1, -1, 1))),
        (((-2, 0), (2, 0), (1, -1), (1, 1)), ((0, 0, 2), (1, -2, 0), (1, 2, 0), (1, 1, -1))),
        (((0, 2),), ((1, 1, 1), (0, -2, 0), (0, 2, 0), (1, 0, 2))),
        (((-1, 2), (-2, -1), (-2, 1)), ((0, -1, -1), (0, 1, -1), (1, -1, 2), (1, -2, -1))),
        (((-3, 0), (3, 0), (2, -1), (2, 1)), ((1, -2, 1), (0, -1, 1), (0, 1, 1), (1, -3, 0))),
        (((1, 2),), ((1, 3, 0), (1, 2, -1), (1, 2, 1), (1, 1, 2))),
        (((-2, 2), (4, 0), (-3, -1), (-3, 1)), ((0, -1, 2), (0, 1, 2), (1, -2, 2), (1, 4, 0))),
        ((), ((1, -3, -1), (1, -3, 1), (0, -3, 0), (0, 3, 0))),
        (((3, -1), (3, 1), (2, 2)), ((0, -2, -1), (0, 2, -1), (1, 3, -1), (1, 3, 1))),
        (((4, -1), (4, 1)), ((1, 2, 2), (0, -2, 1), (0, 2, 1), (1, 4, -1))),
        (((-3, 2),), ((1, 4, 1), (0, -2, 2), (0, 2, 2), (1, -3, 2))),
        (((3, 2), (4, 2)), ((0, 4, 0), (1, 3, 2), (1, 4, 2), (0, -3, -1))),
        ((), ((0, 3, -1), (0, -3, 1), (0, 3, 1), (0, -3, 2))),
        ((), ((0, 3, 2), (0, 4, -1), (0, 4, 1), (0, 4, 2))),
    ),
)


def routes(kind, dz, dx):
    z_way, z_piece = ("z+", "k") if dz < 0 else ("z-", "v")
    z_out = [("b" if abs(dz) < 3 else z_piece, z_way)] if 0 < abs(dz) < 4 else []
    turn = [("k", "x+")] if dx == -1 else [("v", "x-")] if dx == 1 else []
    wide = [("b", "x+"), ("b", "x-")]
    if dz == 0 and dx == 0:
        out = [("b", "z+"), ("b", "z-")] + wide
    elif kind == 0 and dz == 0:
        out = [("b", "z+"), ("b", "z-")] + turn
    elif kind == 0 and dz == 4:
        out = []
    elif kind == 0:
        out = z_out
    else:
        out = z_out + wide if dx == 0 else turn
    return out + [("b", "s")]


def pieces(kind, dz, dx):
    if kind == 0:
        return "kv" if dz == 4 or (dz, dx) == (0, 2) else "b"
    return "kv" if dx == 2 or (dz, dx) == (4, 0) else "b"


def slot_of(kind, dz, dx):
    return (kind * Z + dz % Z) * X + dx % X


def second_sem(kind, dz, dx):
    if kind == 0:
        return 4 if dz == 0 else dx % X
    return 0 if dx == 0 else 1 + dz % Z


def kernel(
    q_ref, k_ref, v_ref, doc_ref, ord_ref, w_ref, own_out, left_in, right_in,
    buf, qin, vin, wbuf, qt, acc, mx, att, part, rin, sums,
    recv, recv2, send, y_send, y_recv, local, w_sem,
):
    cp, tp = lax.axis_index("cp"), lax.axis_index("tp")
    core, x, z = lax.rem(cp, 2), lax.rem(cp // 2, X), cp // (2 * X)

    def at(to):
        if to == "s":
            return (cp + 1 - 2 * core, tp)
        dz, dx = {"z+": (1, 0), "z-": (-1, 0), "x+": (0, 1), "x-": (0, -1)}[to]
        return ((lax.rem(z + dz + Z, Z) * X + lax.rem(x + dx + X, X)) * 2 + core, tp)

    def copy(kind, dz, dx, piece, to):
        mz, mx_ = {"s": (0, 0), "z+": (-1, 0), "z-": (1, 0), "x+": (0, -1), "x-": (0, 1)}[to]
        there = (kind, (dz + mz + 3) % Z - 3, (dx + mx_ + 1) % X - 1)
        here, dest = slot_of(kind, dz, dx), slot_of(*there)
        src, dst, sem = buf.at[here], buf.at[dest], recv.at[dest]
        if piece == "k":
            src, dst = buf.at[here, 0], buf.at[dest, 0]
        elif piece == "v":
            src, dst, sem = buf.at[here, 1], buf.at[dest, 1], recv2.at[second_sem(*there)]
        return pltpu.make_async_remote_copy(
            src_ref=src, dst_ref=dst, send_sem=send, recv_sem=sem, device_id=at(to), device_id_type=MESH_ID
        )

    def arrived(kind, dz, dx, how):
        slot = slot_of(kind, dz, dx)
        for piece in how:
            ref, sem = buf.at[slot], recv.at[slot]
            if piece == "k":
                ref = buf.at[slot, 0]
            elif piece == "v":
                ref, sem = buf.at[slot, 1], recv2.at[second_sem(kind, dz, dx)]
            pltpu.make_async_remote_copy(
                src_ref=ref, dst_ref=ref, send_sem=send, recv_sem=sem, device_id=at("s"), device_id_type=MESH_ID
            ).wait_recv()

    my_slot = core * (Z * X)
    neighbours = [at(to) for to in ("s", "z+", "z-", "x+", "x-")]
    up, down = (cp, lax.rem(tp + 1, TP)), (cp, lax.rem(tp + TP - 1, TP))
    neighbours += [up, down]

    loads = [
        pltpu.make_async_copy(v_ref, vin, local.at[0]),
        pltpu.make_async_copy(k_ref.at[:, 0:HEAD], buf.at[my_slot, 0, 0], local.at[1]),
        pltpu.make_async_copy(k_ref.at[:, HEAD : 2 * HEAD], buf.at[my_slot, 0, 1], local.at[2]),
        pltpu.make_async_copy(q_ref, qin, local.at[3]),
    ]
    for c in loads:
        c.start()
    weights = [
        pltpu.make_async_copy(
            w_ref.at[:, n * COLS : (n + 1) * COLS], wbuf.at[:, n * COLS : (n + 1) * COLS], w_sem.at[n]
        )
        for n in range(NCHUNK)
    ]
    barrier = pltpu.get_barrier_semaphore()
    for device in neighbours:
        pl.semaphore_signal(barrier, inc=1, device_id=device, device_id_type=MESH_ID)
    with jax.named_scope("entry"):
        loads[0].wait()
        for h in range(HKV):
            vt = vin[:, h * HEAD : (h + 1) * HEAD].astype(F32).T.astype(BF16)
            buf[my_slot, 1, h] = vt
        loads[1].wait()
        loads[2].wait()
        pl.semaphore_wait(barrier, len(neighbours))

    for kind in range(2):

        @pl.when(core == kind)
        def _(kind=kind):
            for piece, to in routes(kind, 0, 0):
                copy(kind, 0, 0, piece, to).start()


    with jax.named_scope("queries"):
        loads[3].wait()
        for h in range(HKV):
            for g in range(GROUP):
                i = h * GROUP + g
                scaled = (qin[:, i * HEAD : (i + 1) * HEAD].astype(F32) * SCALE).T
                high = scaled.astype(BF16)
                qt[h, 0:HEAD, g * ROWS : (g + 1) * ROWS] = high
                qt[h, HEAD : 2 * HEAD, g * ROWS : (g + 1) * ROWS] = (scaled - high.astype(F32)).astype(BF16)

    own_seq = ord_ref[cp]
    first_seq, end = jnp.int32(0), jnp.int32(0)
    for d in range(4):
        end = end + doc_ref[d]
        first_seq = jnp.where(end <= own_seq, end, first_seq)

    tiles = [(h, i) for h in range(HKV) for i in range(QL // TILE)]

    key_at = lax.broadcasted_iota(jnp.int32, (ROWS, TILE), 0)
    query_at = lax.rem(lax.broadcasted_iota(jnp.int32, (ROWS, TILE), 1), ROWS)
    seen = key_at <= query_at
    ones = jnp.ones((ONES, ROWS), BF16)
    with jax.named_scope("own"):
        for h, i in tiles:
            lanes = slice(i * TILE, (i + 1) * TILE)
            keys = buf[my_slot, 0, h]
            s = jnp.dot(jnp.concatenate([keys, keys], axis=1), qt[h, :, lanes], preferred_element_type=F32)
            s = jnp.where(seen, s, -FAR)
            m = jnp.max(s, axis=0, keepdims=True)
            p = jnp.exp2(s - m).astype(BF16)
            values = jnp.concatenate([buf[my_slot, 1, h], ones], axis=0)
            acc[h, :, lanes] = jnp.dot(values, p, preferred_element_type=F32)
            mx[h, :, lanes] = m

    more_ones = jnp.ones((ONES, X * ROWS), BF16)

    def attend(slots, biases):
        def scores(h, i):
            keys = jnp.concatenate([buf[slot, 0, h] for slot in slots], axis=0)
            return jnp.dot(
                jnp.concatenate([keys, keys], axis=1),
                qt[h, :, i * TILE : (i + 1) * TILE],
                preferred_element_type=F32,
            )

        def soft(s, h, i):
            lanes = slice(i * TILE, (i + 1) * TILE)
            blocks = [s[j * ROWS : (j + 1) * ROWS] for j in range(X)]
            old = mx[h, :, lanes]
            m = old
            for j in range(X):
                m = jnp.maximum(m, jnp.max(blocks[j], axis=0, keepdims=True) - biases[j])
            mx[h, :, lanes] = m
            p = jnp.concatenate([jnp.exp2(blocks[j] - (m + biases[j])).astype(BF16) for j in range(X)], axis=0)
            return p, jnp.exp2(old - m)

        def add(p, factor, h, i):
            lanes = slice(i * TILE, (i + 1) * TILE)
            values = jnp.concatenate([buf[slot, 1, h] for slot in slots], axis=1)
            values = jnp.concatenate([values, more_ones], axis=0)
            acc[h, :, lanes] = acc[h, :, lanes] * factor + jnp.dot(values, p, preferred_element_type=F32)

        coming, waiting = scores(*tiles[0]), None
        for n, tile in enumerate(tiles):
            s = coming
            if n + 1 < len(tiles):
                coming = scores(*tiles[n + 1])
            if waiting is not None:
                add(*waiting)
            waiting = soft(s, *tile) + tile
        add(*waiting)

    def step(t, carry):
        def dispatch(kind, low, high):
            if high - low > 1:
                middle = (low + high) // 2
                return lax.cond(
                    t < middle, lambda: dispatch(kind, low, middle), lambda: dispatch(kind, middle, high)
                )
            passed, group = PLAN[kind][low]
            with jax.named_scope(f"step{low}"):
                for dz, dx in passed:
                    arrived(kind, dz, dx, pieces(kind, dz, dx))
                    for piece, to in routes(kind, dz, dx):
                        copy(kind, dz, dx, piece, to).start()
            with jax.named_scope(f"sib{low}"):
                for of, dz, dx in group:
                    if of != kind:
                        arrived(of, dz, dx, "b")
            return tuple(jnp.int32(slot_of(*block)) for block in group)

        slots = lax.cond(core == 0, lambda: dispatch(0, 0, 16), lambda: dispatch(1, 0, 16))
        biases = []
        for slot in slots:
            of, dz, dx = slot // (Z * X), lax.rem(slot // X, Z), lax.rem(slot, X)
            seq = ord_ref[(lax.rem(z + dz, Z) * X + lax.rem(x + dx, X)) * 2 + of]
            biases.append(jnp.where((seq >= first_seq) & (seq < own_seq), 0.0, FAR))
        @pl.when(t == 2)
        def _():
            for c in weights:
                c.start()

        with jax.named_scope("attend"):
            attend(slots, biases)
        return carry

    lax.fori_loop(0, 16, step, 0)

    with jax.named_scope("attended"):
        for h in range(HKV):
            for g in range(GROUP):
                lanes = slice(g * ROWS, (g + 1) * ROWS)
                a = acc[h, 0:HEAD, lanes] / acc[h, HEAD : HEAD + 1, lanes]
                i = h * GROUP + g
                att[:, i * HEAD : (i + 1) * HEAD] = a.T.astype(BF16)

    own, above, below, over = tp, up[1], down[1], lax.rem(tp + 2, TP)
    half = NCHUNK // 2
    chunks = [n // 2 + (n % 2) * half for n in range(NCHUNK)]

    def y_copy(src, dst, index, target):
        return pltpu.make_async_remote_copy(
            src_ref=src, dst_ref=dst, send_sem=y_send, recv_sem=y_recv.at[index],
            device_id=target, device_id_type=MESH_ID,
        )

    def cols(n):
        return slice(n * COLS, (n + 1) * COLS)

    def kept(n):
        return pltpu.make_async_copy(part.at[n, own], own_out.at[:, cols(n)], w_sem.at[n])

    def relay(n):
        return y_copy(part.at[n, over], rin.at[n], n, up if n < half else down)

    def direct(n):
        if n < half:
            return y_copy(part.at[n, below], right_in.at[:, cols(n)], NCHUNK + n, down)
        return y_copy(part.at[n, above], left_in.at[:, cols(n)], NCHUNK + n, up)

    def summed(n):
        if n < half:
            return y_copy(sums.at[n], left_in.at[:, cols(n)], 2 * NCHUNK + n, up)
        return y_copy(sums.at[n], right_in.at[:, cols(n)], 2 * NCHUNK + n, down)

    with jax.named_scope("project"):
        attended = att[...]
        ready = None
        for n in chunks:
            weights[n].wait()
            piece = jnp.dot(attended, wbuf[:, n * COLS : (n + 1) * COLS], preferred_element_type=F32)
            part[n] = piece.astype(BF16).reshape(TP, ROWS // TP, COLS)
            if ready is not None:
                relay(ready).start()
                direct(ready).start()
                kept(ready).start()
            ready = n
        relay(ready).start()
        direct(ready).start()
        kept(ready).start()
        ready = None
        for n in chunks:
            relay(n).wait_recv()
            onward = above if n < half else below
            sums[n] = (rin[n].astype(F32) + part[n, onward].astype(F32)).astype(BF16)
            if ready is not None:
                summed(ready).start()
            ready = n
        summed(ready).start()
        for n in chunks:
            direct(n).wait_recv()
            summed(n).wait_recv()

    sent = part.at[0 : 3 * NCHUNK // TP]
    y = pltpu.make_async_remote_copy(
        src_ref=sent, dst_ref=sent, send_sem=y_send, recv_sem=y_recv.at[0], device_id=up, device_id_type=MESH_ID
    )
    y.wait_send()
    sent = buf.at[0 : 2 * Z * X - 1]
    blocks = pltpu.make_async_remote_copy(
        src_ref=sent, dst_ref=sent, send_sem=send, recv_sem=recv.at[0], device_id=at("s"), device_id_type=MESH_ID
    )
    blocks.wait_send()
    for n in range(NCHUNK):
        kept(n).wait()


def local(queries, keys, values, doc_blocks, block_order, out_weight):
    any_, smem = pl.BlockSpec(memory_space=pl.ANY), pl.BlockSpec(memory_space=pltpu.SMEM)
    rows = ROWS // TP
    own, left, right = pl.pallas_call(
        kernel,
        out_shape=[jax.ShapeDtypeStruct((rows, WIN), BF16)] * 3,
        in_specs=[any_, any_, any_, smem, smem, any_],
        out_specs=[any_] * 3,
        scratch_shapes=[
            pltpu.VMEM((2 * Z * X, 2, HKV, ROWS, HEAD), BF16),
            pltpu.VMEM((ROWS, HKV * GROUP * HEAD), BF16),
            pltpu.VMEM((ROWS, HKV * HEAD), BF16),
            pltpu.VMEM((HKV * GROUP * HEAD, WIN), BF16),
            pltpu.VMEM((HKV, 2 * HEAD, QL), BF16),
            pltpu.VMEM((HKV, HEAD + ONES, QL), F32),
            pltpu.VMEM((HKV, 1, QL), F32),
            pltpu.VMEM((ROWS, HKV * GROUP * HEAD), BF16),
            pltpu.VMEM((NCHUNK, TP, rows, COLS), BF16),
            pltpu.VMEM((NCHUNK, rows, COLS), BF16),
            pltpu.VMEM((NCHUNK, rows, COLS), BF16),
            pltpu.SemaphoreType.DMA((2 * Z * X,)),
            pltpu.SemaphoreType.DMA((1 + Z,)),
            pltpu.SemaphoreType.DMA(()),
            pltpu.SemaphoreType.DMA(()),
            pltpu.SemaphoreType.DMA((3 * NCHUNK,)),
            pltpu.SemaphoreType.DMA((4,)),
            pltpu.SemaphoreType.DMA((NCHUNK,)),
        ],
        compiler_params=pltpu.CompilerParams(
            collective_id=0, has_side_effects=True, vmem_limit_bytes=60 * 1024 * 1024
        ),
        name="attention",
    )(queries, keys, values, doc_blocks, block_order, out_weight)
    return (own.astype(F32) + left.astype(F32) + right.astype(F32)).astype(BF16)


def solution(mesh):
    placed = (P("cp", "tp"), P("cp", "tp"), P("cp", "tp"), P(), P(), P("tp", None))
    return jax.shard_map(
        local, mesh=mesh, in_specs=placed, out_specs=P(("cp", "tp"), None), check_vma=False
    )
```
